32 devices in a mesh: grp: 4 (over y, core), mat: 8 (over z, x).
Axes of the slice: x: 2, y: 2, z: 4, core: 2. Of those that a mesh axis runs over, the one named last changes fastest.
Arguments:
- basis_values: bfloat16 [512, 256, 512], P(('grp', 'mat')), may hold values from -6 to 6
- weights: float32 [512, 256], P(('grp', 'mat')), may hold values from 0.004 to 0.04
- density: bfloat16 [192, 5, 128, 128], P('mat'), may hold values from -0.01171875 to 0.01171875
- block_live: int32 [192, 5], P('mat'), may hold values 0 or 1
- batch_blocks: int32 [512, 4], P(('grp', 'mat')), may hold values from 0 to 191, as said below
- live_functions: int32 [512], P(('grp', 'mat')), may hold values from 385 to 512
Outputs:
- site_density: float32 [512, 256], P(('grp', 'mat'))
- hamiltonian: bfloat16 [192, 5, 128, 128], P('mat', None, 'grp')
The draws below stay inside these ranges and needn't reach their ends.
Inputs may be any that keep to these rules, and one draw needn't show every extreme that they name: `batch_blocks`: each row holds 4 increasing blocks within 5 consecutive blocks. The batches of device d are rows d * 16 to d * 16 + 15, counting devices grp first, and all their blocks lie in 8 consecutive block rows, the first of which is used by some batch of the device and the last by another; some batch spans 5 blocks.
All inputs are finite; a program needn't handle non-finite values. No bound on the sum of `block_live` on one device may be relied on, other than what follows from the above.
Results may differ from the reference program's by a relative error of at most 0.0049.
Values may be sent and summed in bfloat16 or wider, within the bound.
No kernel may reach another device: no remote copies, remote signals or barrier semaphores. Data moves between devices by JAX's collectives and lax.ppermute only.
A program may use at most 128 MiB of HBM per device.

```python
import math
import jax
import jax.numpy as jnp
from jax import lax

BLK = 128
NBB = 4
PTS = 256
KB_DEV = 24
BAT_DEV = 16
SPAN = 5
REGION = 8
KB = 192
BATCHES = 512
N_MAT = 8


def layout(key):
    folded = jax.random.fold_in(key, 4242)
    key_first, key_shift, key_skip = jax.random.split(folded, 3)
    devices_count = BATCHES // BAT_DEV
    firsts = jax.random.randint(key_first, (devices_count,), 0, KB - REGION + 1)
    shifts = jax.random.randint(key_shift, (devices_count, BAT_DEV), 0, REGION - SPAN + 1)
    batch_index = jnp.arange(BAT_DEV)[None, :]
    shifts = jnp.where(batch_index == 0, 0, jnp.where(batch_index == 1, REGION - SPAN, shifts))
    skipped = jax.random.randint(key_skip, (devices_count, BAT_DEV), 0, SPAN)
    skipped = jnp.where(batch_index < 2, 1 + skipped % (SPAN - 2), skipped)
    window = firsts[:, None] + shifts
    slot_index = jnp.arange(NBB)
    blocks = window[:, :, None] + slot_index + (slot_index >= skipped[:, :, None]).astype(jnp.int32)
    return blocks.reshape(BATCHES, NBB).astype(jnp.int32)


def draw_batch_blocks(key, part):
    return layout(key)


def with_ends(drawn, rng, least, largest):
    longest = drawn.shape.index(max(drawn.shape))
    spots = []
    for shift in (0, 1):
        where = [jax.random.randint(jax.random.fold_in(rng, axis), (), 0, length) for axis, length in enumerate(drawn.shape)]
        where[longest] = (where[longest] + shift) % drawn.shape[longest]
        spots.append(tuple(where))
    return drawn.at[spots[0]].set(least).at[spots[1]].set(largest)


def block_scale(stream_key, extent, cuts, smallest, high):
    def one(dim, blocks):
        steps = jax.random.uniform(jax.random.fold_in(jax.random.fold_in(stream_key, 6), dim), (blocks,), jnp.float32, smallest / len(cuts), high / len(cuts))
        return jnp.repeat(jnp.exp(steps), extent[dim] // blocks).reshape((-1,) + (1,) * (len(extent) - dim - 1))

    factor_of = one(*cuts[0])
    for cut in cuts[1:]:
        factor_of = factor_of * one(*cut)
    return factor_of


def centred(key, extent, spread, reach, cuts=(), held_as=jnp.bfloat16):
    drawn = spread * jax.random.normal(key, extent, jnp.float32)
    if cuts:
        drawn = drawn * block_scale(key, extent, cuts, -0.22, 0.18)
    return jnp.clip(drawn, -reach, reach).astype(held_as)


def setup_inputs(seed: int = 0) -> dict:
    streams_of = jax.random.split(jax.random.key(seed), 7)
    return {
        "basis_values": centred(streams_of[0], (BATCHES, PTS, NBB * BLK), 1.0, 6.0, ((0, 32),)),
        "weights": jnp.clip(jnp.exp(math.log(0.04) - 2.30258502 * jax.random.uniform(streams_of[1], (BATCHES, PTS), jnp.float32) ** block_scale(streams_of[1], (BATCHES, PTS), ((0, 32),), -0.2, 0.2)), 0.004, 0.04),
        "density": centred(streams_of[2], (KB, SPAN, BLK, BLK), (1.0 / (NBB * BLK)), 0.01171875, ((0, 8),)),
        "block_live": with_ends((jax.random.randint(streams_of[3], (KB, SPAN), 0, 8) < 7).astype(jnp.int32), jax.random.fold_in(streams_of[3], 1), 0, 1),
        "batch_blocks": draw_batch_blocks(jax.random.fold_in(streams_of[6], 71), 0),
        "live_functions": with_ends(jax.random.randint(streams_of[5], (BATCHES,), (NBB - 1) * BLK + 1, NBB * BLK + 1), jax.random.fold_in(streams_of[5], 1), (NBB - 1) * BLK + 1, NBB * BLK).astype(jnp.int32),
    }


def stored_row(block_index):
    return block_index % N_MAT * KB_DEV + block_index // N_MAT

def reference(basis_values, weights, density, block_live, batch_blocks, live_functions):
    masked_density = density * block_live.astype(jnp.bfloat16)[:, :, None, None]
    batch_width = NBB * BLK
    function_index = jnp.arange(batch_width).astype(jnp.int32)
    slot_index = jnp.arange(NBB)
    upper_half = slot_index[:, None] <= slot_index[None, :]
    step_inputs = (basis_values.reshape(BATCHES // 4, 4, PTS, batch_width), weights.reshape(BATCHES // 4, 4, PTS), batch_blocks.reshape(BATCHES // 4, 4, NBB), live_functions.reshape(BATCHES // 4, 4))

    def integrate(ham_total, inputs):
        values, point_weights, blocks, live_count = inputs
        values = jnp.where(function_index[None, None, :] < live_count[:, None, None], values, jnp.zeros_like(values))
        lower_block = jnp.minimum(blocks[:, :, None], blocks[:, None, :])
        upper_block = jnp.maximum(blocks[:, :, None], blocks[:, None, :])
        row_index = stored_row(lower_block).astype(jnp.int32)
        offset = (upper_block - lower_block).astype(jnp.int32)
        gathered_tiles = masked_density[row_index, offset]
        gathered_tiles = jnp.where(upper_half[None, :, :, None, None], gathered_tiles, jnp.swapaxes(gathered_tiles, -1, -2))
        batch_matrix = gathered_tiles.transpose(0, 1, 3, 2, 4).reshape(4, batch_width, batch_width)
        values_wide = values.astype(jnp.float32)
        product_rows = jnp.einsum('brf,bfg->brg', values_wide, batch_matrix.astype(jnp.float32))
        site_values = lax.optimization_barrier(jnp.sum(product_rows * values_wide, axis=-1))
        potential = point_weights * site_values / jnp.sqrt(1.0 + site_values * site_values)
        weighted = (potential[:, :, None] * values_wide).astype(jnp.bfloat16)
        ham_batch = jnp.einsum('brf,brg->bfg', values_wide, weighted.astype(jnp.float32))
        ham_tiles = ham_batch.reshape(4, NBB, BLK, NBB, BLK).transpose(0, 1, 3, 2, 4)
        increment = jnp.where(upper_half[None, :, :, None, None], ham_tiles, jnp.zeros_like(ham_tiles))
        ham_total = ham_total.at[row_index, offset].add(increment)
        return (ham_total, site_values)
    ham_total, site_values = lax.scan(integrate, jnp.zeros((KB, SPAN, BLK, BLK), jnp.float32), step_inputs)
    hamiltonian = (ham_total * block_live.astype(jnp.float32)[:, :, None, None]).astype(jnp.bfloat16)
    return (site_values.reshape(BATCHES, PTS), hamiltonian)
```

```python
import functools

import jax
import jax.numpy as jnp
from jax import lax
from jax.experimental import pallas as pl
from jax.experimental.pallas import tpu as pltpu
from jax.sharding import PartitionSpec as P

MIB = 1 << 20


def pick_kernel(rows, live, density, out, sems):
    count, span = out.shape[0], out.shape[1]

    def copy(d):
        return pltpu.make_async_copy(density.at[rows[d]], out.at[d], sems.at[d])

    for d in range(count):
        copy(d).start()

    def scale(d, carry):
        copy(d).wait()
        for o in range(span):
            factor = (live[rows[d], o] * (1 if o == 0 else 2)).astype(jnp.float32)
            out[d, o] = (out[d, o].astype(jnp.float32) * factor).astype(jnp.bfloat16)
        return carry

    lax.fori_loop(0, count, scale, 0)


def pick_rows(rows, live, density):
    count = rows.shape[0]
    return pl.pallas_call(
        pick_kernel,
        out_shape=jax.ShapeDtypeStruct((count,) + density.shape[1:], jnp.bfloat16),
        in_specs=[
            pl.BlockSpec(memory_space=pltpu.SMEM),
            pl.BlockSpec(memory_space=pltpu.SMEM),
            pl.BlockSpec(memory_space=pl.ANY),
        ],
        out_specs=pl.BlockSpec(memory_space=pltpu.VMEM),
        scratch_shapes=[pltpu.SemaphoreType.DMA((count,))],
        compiler_params=pltpu.CompilerParams(vmem_limit_bytes=16 * MIB),
        name="pick",
    )(rows, live, density)


def turn_kernel(live, values, out):
    batch = pl.program_id(0)
    turned = values[0].astype(jnp.float32).T
    index = lax.broadcasted_iota(jnp.int32, turned.shape, 0)
    out[0] = jnp.where(index < live[batch], turned, 0.0).astype(jnp.bfloat16)


def turn_values(live, values):
    batches, points, width = values.shape
    return pl.pallas_call(
        turn_kernel,
        out_shape=jax.ShapeDtypeStruct((batches, width, points), jnp.bfloat16),
        grid_spec=pltpu.PrefetchScalarGridSpec(
            num_scalar_prefetch=1,
            grid=(batches,),
            in_specs=[pl.BlockSpec((1, points, width), lambda b, live: (b, 0, 0))],
            out_specs=pl.BlockSpec((1, width, points), lambda b, live: (b, 0, 0)),
        ),
        compiler_params=pltpu.CompilerParams(vmem_limit_bytes=16 * MIB),
        cost_estimate=pl.CostEstimate(
            flops=20_000_000_000, bytes_accessed=4 * batches * points * width, transcendentals=0
        ),
        name="turn",
    )(live, values)


def integrate_kernel(groups, blocks, turned, weights, region, site_out, pieces, matrix, total):
    holders, span, block, _ = region.shape
    batches, width, points = turned.shape
    slots = width // block
    half = width // 2
    matrix[...] = jnp.zeros_like(matrix)
    total[...] = jnp.zeros_like(total)

    def one(b, carry):
        ids = [blocks[b, k] for k in range(slots)]
        homes = [lax.rem(i, holders) for i in ids]
        pairs = [(k, l) for k in range(slots) for l in range(k, slots)]
        for k, l in pairs:
            matrix[k * block : (k + 1) * block, l * block : (l + 1) * block] = region[
                homes[k], ids[l] - ids[k]
            ]
        values = turned[b]
        lower = values[half:]
        product_top = jnp.dot(matrix[:half, :], values, preferred_element_type=jnp.float32)
        product_low = jnp.dot(matrix[half:, half:], lower, preferred_element_type=jnp.float32)
        wide = values.astype(jnp.float32)
        site = jnp.sum(product_top * wide[:half] + product_low * wide[half:], axis=0, keepdims=True)
        site_out[pl.ds(b, 1), :] = site
        potential = weights[pl.ds(b, 1), :] * site / jnp.sqrt(1.0 + site * site)
        weighted = (potential * wide).astype(jnp.bfloat16)
        rows = (((1,), (1,)), ((), ()))
        ham_top = lax.dot_general(values[:half], weighted, rows, preferred_element_type=jnp.float32)
        ham_low = lax.dot_general(lower, weighted[half:], rows, preferred_element_type=jnp.float32)
        for k, l in pairs:
            low = k * block >= half
            source, column = (ham_low, l * block - half) if low else (ham_top, l * block)
            row = k * block - half if low else k * block
            total[homes[k], ids[l] - ids[k]] += source[row : row + block, column : column + block]
        return carry

    lax.fori_loop(0, batches, one, 0)
    part = block // groups

    def store(h, carry):
        for g in range(groups):
            for o in range(span):
                pieces[g * holders + h, o] = total[h, o, g * part : (g + 1) * part, :].astype(
                    jnp.bfloat16
                )
        return carry

    lax.fori_loop(0, holders, store, 0)


def integrate(groups, blocks, turned, weights, region):
    batches, width, points = turned.shape
    holders, span, block, _ = region.shape
    vmem = pl.BlockSpec(memory_space=pltpu.VMEM)
    return pl.pallas_call(
        functools.partial(integrate_kernel, groups),
        out_shape=(
            jax.ShapeDtypeStruct((batches, points), jnp.float32),
            jax.ShapeDtypeStruct((groups * holders, span, block // groups, block), jnp.bfloat16),
        ),
        in_specs=[pl.BlockSpec(memory_space=pltpu.SMEM), vmem, vmem, vmem],
        out_specs=(vmem, vmem),
        scratch_shapes=[
            pltpu.VMEM((width, width), jnp.bfloat16),
            pltpu.VMEM((holders, span, block, block), jnp.float32),
        ],
        compiler_params=pltpu.CompilerParams(vmem_limit_bytes=40 * MIB),
        name="integrate",
    )(blocks, turned, weights, region)


def finish_kernel(rows, live, arrived, out, total):
    sources, span = arrived.shape[0], arrived.shape[1]
    local = out.shape[0]
    total[...] = jnp.zeros_like(total)

    def add(s, carry):
        total[rows[s]] += arrived[s].astype(jnp.float32)
        return carry

    lax.fori_loop(0, sources, add, 0)

    def store(t, carry):
        for o in range(span):
            out[t, o] = (total[t, o] * live[t, o].astype(jnp.float32)).astype(jnp.bfloat16)
        return carry

    lax.fori_loop(0, local, store, 0)


def finish(rows, live, arrived):
    local = live.shape[0]
    shape = (local,) + arrived.shape[1:]
    smem = pl.BlockSpec(memory_space=pltpu.SMEM)
    vmem = pl.BlockSpec(memory_space=pltpu.VMEM)
    return pl.pallas_call(
        finish_kernel,
        out_shape=jax.ShapeDtypeStruct(shape, jnp.bfloat16),
        in_specs=[smem, smem, vmem],
        out_specs=vmem,
        scratch_shapes=[pltpu.VMEM(shape, jnp.float32)],
        compiler_params=pltpu.CompilerParams(vmem_limit_bytes=24 * MIB),
        name="finish",
    )(rows, live, arrived)


def per_device(basis_values, weights, density, block_live, batch_blocks, live_functions):
    holders = lax.axis_size("mat")
    groups = lax.axis_size("grp")
    holder = lax.axis_index("mat")
    first = jnp.min(batch_blocks)
    firsts = lax.psum(jnp.where(jnp.arange(holders) == holder, first, 0), "mat")
    wanted = (firsts + (holder - firsts) % holders - holder) // holders
    outgoing = pick_rows(wanted, block_live, density)
    region = lax.all_to_all(outgoing, "mat", split_axis=0, concat_axis=0, tiled=True)
    turned = turn_values(live_functions, basis_values)
    all_rows = lax.all_gather(wanted, "grp", axis=0, tiled=True)
    site_density, pieces = integrate(groups, batch_blocks, turned, weights, region)
    arrived = lax.all_to_all(pieces, ("grp", "mat"), split_axis=0, concat_axis=0, tiled=True)
    hamiltonian = finish(all_rows, block_live, arrived)
    return site_density, hamiltonian


def solution(mesh):
    in_specs = (
        P(("grp", "mat"), None, None),
        P(("grp", "mat"), None),
        P("mat", None, None, None),
        P("mat", None),
        P(("grp", "mat"), None),
        P(("grp", "mat")),
    )
    out_specs = (P(("grp", "mat"), None), P("mat", None, "grp", None))
    return jax.shard_map(
        per_device, mesh=mesh, in_specs=in_specs, out_specs=out_specs, check_vma=False
    )
```

```python
import functools

import jax
import jax.numpy as jnp
from jax import lax
from jax.experimental import pallas as pl
from jax.experimental.pallas import tpu as pltpu
from jax.sharding import PartitionSpec as P


MIB = 1 << 20
NEAR = 3


def local_row(first, holder, holders):
    return lax.div(first + lax.rem(holder - lax.rem(first, holders) + holders, holders), holders)


def pick_kernel(firsts, live, density, *refs):
    outs, sems = refs[:-1], refs[-1]
    count = len(outs) // 2
    near, far = outs[:count], outs[count:]
    holder = lax.axis_index("mat")
    copies, rows = [], []
    for s in range(count):
        row = local_row(firsts[lax.rem(holder + s, count)], holder, count)
        source = density.at[row]
        rows.append(row)
        copies.append(
            (
                pltpu.make_async_copy(source.at[pl.ds(0, NEAR)], near[s], sems.at[0, s]),
                pltpu.make_async_copy(
                    source.at[pl.ds(NEAR, density.shape[1] - NEAR)], far[s], sems.at[1, s]
                ),
            )
        )
    for part in (0, 1):
        for pair in copies:
            pair[part].start()
    for part, refs_of in ((0, near), (1, far)):
        for s in range(count):
            copies[s][part].wait()
            for j in range(refs_of[s].shape[0]):
                o = j + part * NEAR
                factor = (live[o, rows[s]] * (1 if o == 0 else 2)).astype(jnp.float32)
                refs_of[s][j] = (refs_of[s][j].astype(jnp.float32) * factor).astype(jnp.bfloat16)


def pick_rows(firsts, live, density):
    count = firsts.shape[0]
    smem = pl.BlockSpec(memory_space=pltpu.SMEM)
    vmem = pl.BlockSpec(memory_space=pltpu.VMEM)
    near = jax.ShapeDtypeStruct((NEAR,) + density.shape[2:], jnp.bfloat16)
    far = jax.ShapeDtypeStruct((density.shape[1] - NEAR,) + density.shape[2:], jnp.bfloat16)
    outs = pl.pallas_call(
        pick_kernel,
        out_shape=(near,) * count + (far,) * count,
        in_specs=[smem, smem, pl.BlockSpec(memory_space=pltpu.HBM)],
        out_specs=(vmem,) * (2 * count),
        scratch_shapes=[pltpu.SemaphoreType.DMA((2, count))],
        compiler_params=pltpu.CompilerParams(vmem_limit_bytes=62 * MIB),
        name="pick",
    )(firsts, live, density)
    return outs[:count], outs[count:]


def turn_kernel(live, values, out):
    batch = pl.program_id(0)
    turned = values[0].astype(jnp.float32).T
    index = lax.broadcasted_iota(jnp.int32, turned.shape, 0)
    out[0] = jnp.where(index < live[batch], turned, 0.0).astype(jnp.bfloat16)


def turn_values(live, values):
    batches, points, width = values.shape
    return pl.pallas_call(
        turn_kernel,
        out_shape=jax.ShapeDtypeStruct((batches, width, points), jnp.bfloat16),
        grid_spec=pltpu.PrefetchScalarGridSpec(
            num_scalar_prefetch=1,
            grid=(batches,),
            in_specs=[pl.BlockSpec((1, points, width), lambda b, live: (b, 0, 0))],
            out_specs=pl.BlockSpec((1, width, points), lambda b, live: (b, 0, 0)),
        ),
        compiler_params=pltpu.CompilerParams(vmem_limit_bytes=16 * MIB),
        cost_estimate=pl.CostEstimate(
            flops=20_000_000_000, bytes_accessed=4 * batches * points * width, transcendentals=0
        ),
        name="turn",
    )(live, values)


def unroll_of(batches):
    return next(u for u in (4, 2, 1) if batches % u == 0)


def gather_region(parts, region):
    count = len(parts)
    holder = lax.axis_index("mat")
    for s in range(count):
        region[lax.rem(holder - s + count, count)] = parts[s][...]


def where_is(blocks, b, slots, holders):
    ids = [blocks[k, b] for k in range(slots)]
    return ids, [lax.rem(i, holders) for i in ids]


def join(rows):
    return jnp.concatenate([jnp.concatenate(row, axis=1) for row in rows], axis=0)


def near_kernel(blocks, turned, *refs):
    parts, site_out, region = refs[:-2], refs[-2], refs[-1]
    holders, _, block, _ = region.shape
    batches, width, _ = turned.shape
    slots = width // block
    half = width // 2
    unroll = unroll_of(batches)
    gather_region(parts, region)
    zero = jnp.zeros((block, block), jnp.bfloat16)

    def density_of(b):
        ids, homes = where_is(blocks, b, slots, holders)

        def tile(k, l):
            if k > l or l - k >= NEAR:
                return zero
            offset = ids[l] - ids[k]
            if l - k + 1 < NEAR:
                return region[homes[k], offset]
            stored = region[homes[k], jnp.minimum(offset, NEAR - 1)]
            return jnp.where(offset < NEAR, stored, zero)

        def tiles(rows, columns):
            return join([[tile(k, l) for l in columns] for k in rows])

        values = turned[b]
        top = tiles(range(slots // 2), range(slots))
        low = tiles(range(slots // 2, slots), range(slots // 2, slots))
        product_top = jnp.dot(top, values, preferred_element_type=jnp.float32)
        product_low = jnp.dot(low, values[half:], preferred_element_type=jnp.float32)
        wide = values.astype(jnp.float32)
        site_out[pl.ds(b, 1), :] = jnp.sum(
            product_top * wide[:half] + product_low * wide[half:], axis=0, keepdims=True
        )

    def densities(step, carry):
        for u in range(unroll):
            density_of(step * unroll + u)
        return carry

    lax.fori_loop(0, batches // unroll, densities, 0)


def near_density(blocks, turned, parts):
    batches, _, points = turned.shape
    vmem = pl.BlockSpec(memory_space=pltpu.VMEM)
    return pl.pallas_call(
        near_kernel,
        out_shape=jax.ShapeDtypeStruct((batches, points), jnp.float32),
        in_specs=[pl.BlockSpec(memory_space=pltpu.SMEM)] + [vmem] * (1 + len(parts)),
        out_specs=vmem,
        scratch_shapes=[pltpu.VMEM((len(parts),) + parts[0].shape, jnp.bfloat16)],
        compiler_params=pltpu.CompilerParams(vmem_limit_bytes=24 * MIB),
        cost_estimate=pl.CostEstimate(
            flops=3_000_000_000, bytes_accessed=8_000_000, transcendentals=0
        ),
        name="near_density",
    )(blocks, turned, *parts)


def integrate_kernel(groups, blocks, turned, weights, near_site, *refs):
    parts = refs[:-5]
    site_out, pieces, region, total, potential = refs[-5:]
    holders, far, block, _ = region.shape
    span = far + NEAR
    batches, width, _ = turned.shape
    slots = width // block
    half = width // 2
    unroll = unroll_of(batches)
    pairs = [(k, l) for k in range(slots) for l in range(k, slots)]
    gather_region(parts, region)
    total[...] = jnp.zeros_like(total)
    zero = jnp.zeros((block, block), jnp.bfloat16)

    def density_of(b):
        ids, homes = where_is(blocks, b, slots, holders)

        def tile(k, l):
            if l - k + 1 < NEAR:
                return zero
            offset = ids[l] - ids[k]
            stored = region[homes[k], jnp.maximum(offset - NEAR, 0)]
            return jnp.where(offset >= NEAR, stored, zero)

        lower = turned[b, half:]
        corner = join(
            [[tile(k, l) for l in range(slots // 2, slots)] for k in range(slots // 2)]
        )
        product = jnp.dot(corner, lower, preferred_element_type=jnp.float32)
        site_out[pl.ds(b, 1), :] = near_site[pl.ds(b, 1), :] + jnp.sum(
            product * turned[b, :half].astype(jnp.float32), axis=0, keepdims=True
        )

    def densities(step, carry):
        for u in range(unroll):
            density_of(step * unroll + u)
        return carry

    lax.fori_loop(0, batches // unroll, densities, 0)
    site = site_out[...]
    potential[...] = weights[...] * site / jnp.sqrt(1.0 + site * site)

    def ham_of(b):
        ids, homes = where_is(blocks, b, slots, holders)
        values = turned[b]
        weighted = (potential[pl.ds(b, 1), :] * values.astype(jnp.float32)).astype(jnp.bfloat16)
        over_points = (((1,), (1,)), ((), ()))
        top = lax.dot_general(
            values[:half], weighted, over_points, preferred_element_type=jnp.float32
        )
        low = lax.dot_general(
            values[half:], weighted[half:], over_points, preferred_element_type=jnp.float32
        )
        for k, l in pairs:
            in_low = k * block >= half
            source, column = (low, l * block - half) if in_low else (top, l * block)
            row = k * block - half if in_low else k * block
            total[homes[k], ids[l] - ids[k]] += source[row : row + block, column : column + block]

    def hams(step, carry):
        for u in range(unroll):
            ham_of(step * unroll + u)
        return carry

    lax.fori_loop(0, batches // unroll, hams, 0)
    part = block // groups

    def store(h, carry):
        for g in range(groups):
            for o in range(span):
                pieces[g * holders + h, o] = total[h, o, g * part : (g + 1) * part, :].astype(
                    jnp.bfloat16
                )
        return carry

    lax.fori_loop(0, holders, store, 0)


def integrate(groups, blocks, turned, weights, near_site, parts):
    batches, _, points = turned.shape
    holders = len(parts)
    far, block, _ = parts[0].shape
    span = NEAR + far
    vmem = pl.BlockSpec(memory_space=pltpu.VMEM)
    return pl.pallas_call(
        functools.partial(integrate_kernel, groups),
        out_shape=(
            jax.ShapeDtypeStruct((batches, points), jnp.float32),
            jax.ShapeDtypeStruct((groups * holders, span, block // groups, block), jnp.bfloat16),
        ),
        in_specs=[pl.BlockSpec(memory_space=pltpu.SMEM)] + [vmem] * (3 + holders),
        out_specs=(vmem, vmem),
        scratch_shapes=[
            pltpu.VMEM((holders, far, block, block), jnp.bfloat16),
            pltpu.VMEM((holders, span, block, block), jnp.float32),
            pltpu.VMEM((batches, points), jnp.float32),
        ],
        compiler_params=pltpu.CompilerParams(vmem_limit_bytes=32 * MIB),
        cost_estimate=pl.CostEstimate(
            flops=5_000_000_000, bytes_accessed=8_000_000, transcendentals=0
        ),
        name="integrate",
    )(blocks, turned, weights, near_site, *parts)


def finish_kernel(firsts, live, arrived, out, total):
    sources, span = arrived.shape[0], arrived.shape[1]
    local = out.shape[0]
    holders = lax.axis_size("mat")
    holder = lax.axis_index("mat")
    total[...] = jnp.zeros_like(total)

    def add(s, carry):
        total[local_row(firsts[s], holder, holders)] += arrived[s].astype(jnp.float32)
        return carry

    lax.fori_loop(0, sources, add, 0)

    def store(t, carry):
        for o in range(span):
            out[t, o] = (total[t, o] * live[o, t].astype(jnp.float32)).astype(jnp.bfloat16)
        return carry

    lax.fori_loop(0, local, store, 0)


def finish(firsts, live, arrived):
    shape = (live.shape[1],) + arrived.shape[1:]
    smem = pl.BlockSpec(memory_space=pltpu.SMEM)
    vmem = pl.BlockSpec(memory_space=pltpu.VMEM)
    return pl.pallas_call(
        finish_kernel,
        out_shape=jax.ShapeDtypeStruct(shape, jnp.bfloat16),
        in_specs=[smem, smem, vmem],
        out_specs=vmem,
        scratch_shapes=[pltpu.VMEM(shape, jnp.float32)],
        compiler_params=pltpu.CompilerParams(vmem_limit_bytes=24 * MIB),
        name="finish",
    )(firsts, live, arrived)


def per_device(basis_values, weights, density, block_live, batch_blocks, live_functions):
    holders = lax.axis_size("mat")
    groups = lax.axis_size("grp")
    blocks = batch_blocks.T
    live = block_live.T
    mine = jnp.arange(holders) == lax.axis_index("mat")
    largest = jnp.iinfo(jnp.int32).max
    own = jnp.min(jnp.where(mine[:, None, None], blocks[None], largest), axis=(1, 2))
    firsts = lax.pmin(own, "mat")
    near, far = pick_rows(firsts, live, density)

    def passed_on(parts):
        arrived = [parts[0]]
        for s in range(1, holders):
            shift = [(h, (h + s) % holders) for h in range(holders)]
            arrived.append(lax.ppermute(parts[s], "mat", shift))
        return arrived

    near, far = passed_on(near), passed_on(far)
    turned = turn_values(live_functions, basis_values)
    my_group = jnp.arange(groups) == lax.axis_index("grp")
    all_firsts = lax.psum(jnp.where(my_group[:, None], firsts[None], 0).reshape(-1), "grp")
    near_site = near_density(blocks, turned, near)
    site_density, pieces = integrate(groups, blocks, turned, weights, near_site, far)
    arrived = lax.all_to_all(pieces, ("grp", "mat"), split_axis=0, concat_axis=0, tiled=True)
    hamiltonian = finish(all_firsts, live, arrived)
    return site_density, hamiltonian


def solution(mesh):
    in_specs = (
        P(("grp", "mat"), None, None),
        P(("grp", "mat"), None),
        P("mat", None, None, None),
        P("mat", None),
        P(("grp", "mat"), None),
        P(("grp", "mat")),
    )
    out_specs = (P(("grp", "mat"), None), P("mat", None, "grp", None))
    return jax.shard_map(
        per_device, mesh=mesh, in_specs=in_specs, out_specs=out_specs, check_vma=False
    )
```

```python
import functools

import jax
import jax.numpy as jnp
from jax import lax
from jax.experimental import pallas as pl
from jax.experimental.pallas import tpu as pltpu
from jax.sharding import PartitionSpec as P


MIB = 1 << 20
PICK_LIMIT = 62 * MIB


def local_row(first, holder, holders):
    return lax.div(first + lax.rem(holder - lax.rem(first, holders) + holders, holders), holders)


def pick_kernel(firsts, live, density, *refs):
    outs, sems = refs[:-1], refs[-1]
    count = len(outs)
    holder = lax.axis_index("mat")
    rows = [local_row(firsts[lax.rem(holder + s, count)], holder, count) for s in range(count)]
    copies = [
        pltpu.make_async_copy(density.at[rows[s]], outs[s], sems.at[s]) for s in range(count)
    ]
    for copy in copies:
        copy.start()
    for s in range(count):
        copies[s].wait()
        for o in range(density.shape[1]):
            factor = (live[o, rows[s]] * (1 if o == 0 else 2)).astype(jnp.float32)
            outs[s][o] = (outs[s][o].astype(jnp.float32) * factor).astype(jnp.bfloat16)


def pick_rows(firsts, live, density):
    count = firsts.shape[0]
    smem = pl.BlockSpec(memory_space=pltpu.SMEM)
    vmem = pl.BlockSpec(memory_space=pltpu.VMEM)
    return pl.pallas_call(
        pick_kernel,
        out_shape=(jax.ShapeDtypeStruct(density.shape[1:], jnp.bfloat16),) * count,
        in_specs=[smem, smem, pl.BlockSpec(memory_space=pltpu.HBM)],
        out_specs=(vmem,) * count,
        scratch_shapes=[pltpu.SemaphoreType.DMA((count,))],
        compiler_params=pltpu.CompilerParams(vmem_limit_bytes=PICK_LIMIT),
        name="pick",
    )(firsts, live, density)


def turn_kernel(live, values, out):
    batch = pl.program_id(0)
    turned = values[0].T
    index = lax.broadcasted_iota(jnp.int32, turned.shape, 0)
    out[0] = jnp.where(index < live[batch], turned, jnp.zeros_like(turned))


def turn_values(live, values):
    batches, points, width = values.shape
    return pl.pallas_call(
        turn_kernel,
        out_shape=jax.ShapeDtypeStruct((batches, width, points), jnp.bfloat16),
        grid_spec=pltpu.PrefetchScalarGridSpec(
            num_scalar_prefetch=1,
            grid=(batches,),
            in_specs=[pl.BlockSpec((1, points, width), lambda b, live: (b, 0, 0))],
            out_specs=pl.BlockSpec((1, width, points), lambda b, live: (b, 0, 0)),
        ),
        compiler_params=pltpu.CompilerParams(vmem_limit_bytes=16 * MIB),
        cost_estimate=pl.CostEstimate(
            flops=20_000_000_000, bytes_accessed=4 * batches * points * width, transcendentals=0
        ),
        name="turn",
    )(live, values)


def unroll_of(batches):
    return next(u for u in (8, 4, 2, 1) if batches % u == 0)


def join(rows):
    return jnp.concatenate([jnp.concatenate(row, axis=1) for row in rows], axis=0)


def integrate_kernel(groups, blocks, turned, weights, *refs):
    parts = refs[:-5]
    site_out, pieces, region, total, potential = refs[-5:]
    holders, span, block, _ = region.shape
    batches, width, _ = turned.shape
    slots = width // block
    half = width // 2
    pairs = [(k, l) for k in range(slots) for l in range(k, slots)]
    holder = lax.axis_index("mat")
    for s in range(holders):
        region[lax.rem(holder - s + holders, holders)] = parts[s][...]
    total[...] = jnp.zeros_like(total)
    zero = jnp.zeros((block, block), jnp.bfloat16)

    def where_is(b):
        ids = [blocks[k, b] for k in range(slots)]
        return ids, [lax.rem(i, holders) for i in ids]

    def density_of(b):
        ids, homes = where_is(b)

        def tiles(rows, columns):
            return join(
                [
                    [zero if k > l else region[homes[k], ids[l] - ids[k]] for l in columns]
                    for k in rows
                ]
            )

        values = turned[b]
        top = tiles(range(slots // 2), range(slots))
        low = tiles(range(slots // 2, slots), range(slots // 2, slots))
        product_top = jnp.dot(top, values, preferred_element_type=jnp.float32)
        product_low = jnp.dot(low, values[half:], preferred_element_type=jnp.float32)
        wide = values.astype(jnp.float32)
        site_out[pl.ds(b, 1), :] = jnp.sum(
            product_top * wide[:half] + product_low * wide[half:], axis=0, keepdims=True
        )

    unroll = unroll_of(batches)

    def densities(step, carry):
        for u in range(unroll):
            density_of(step * unroll + u)
        return carry

    lax.fori_loop(0, batches // unroll, densities, 0)
    site = site_out[...]
    potential[...] = weights[...] * site / jnp.sqrt(1.0 + site * site)

    def ham_of(b):
        ids, homes = where_is(b)
        values = turned[b]
        weighted = (potential[pl.ds(b, 1), :] * values.astype(jnp.float32)).astype(jnp.bfloat16)
        over_points = (((1,), (1,)), ((), ()))
        top = lax.dot_general(
            values[:half], weighted, over_points, preferred_element_type=jnp.float32
        )
        low = lax.dot_general(
            values[half:], weighted[half:], over_points, preferred_element_type=jnp.float32
        )
        for k, l in pairs:
            in_low = k * block >= half
            source, column = (low, l * block - half) if in_low else (top, l * block)
            row = k * block - half if in_low else k * block
            total[homes[k], ids[l] - ids[k]] += source[row : row + block, column : column + block]

    def hams(step, carry):
        for u in range(unroll):
            ham_of(step * unroll + u)
        return carry

    lax.fori_loop(0, batches // unroll, hams, 0)
    part = block // groups

    def store(h, carry):
        for g in range(groups):
            for o in range(span):
                pieces[g * holders + h, o] = total[h, o, g * part : (g + 1) * part, :].astype(
                    jnp.bfloat16
                )
        return carry

    lax.fori_loop(0, holders, store, 0)


def integrate(groups, blocks, turned, weights, parts):
    batches, _, points = turned.shape
    holders = len(parts)
    span, block, _ = parts[0].shape
    vmem = pl.BlockSpec(memory_space=pltpu.VMEM)
    return pl.pallas_call(
        functools.partial(integrate_kernel, groups),
        out_shape=(
            jax.ShapeDtypeStruct((batches, points), jnp.float32),
            jax.ShapeDtypeStruct((groups * holders, span, block // groups, block), jnp.bfloat16),
        ),
        in_specs=[pl.BlockSpec(memory_space=pltpu.SMEM)] + [vmem] * (2 + holders),
        out_specs=(vmem, vmem),
        scratch_shapes=[
            pltpu.VMEM((holders, span, block, block), jnp.bfloat16),
            pltpu.VMEM((holders, span, block, block), jnp.float32),
            pltpu.VMEM((batches, points), jnp.float32),
        ],
        compiler_params=pltpu.CompilerParams(vmem_limit_bytes=36 * MIB),
        cost_estimate=pl.CostEstimate(
            flops=5_000_000_000, bytes_accessed=8_000_000, transcendentals=0
        ),
        name="integrate",
    )(blocks, turned, weights, *parts)


def finish_kernel(firsts, live, arrived, out, total):
    sources, span = arrived.shape[0], arrived.shape[1]
    local = out.shape[0]
    holders = lax.axis_size("mat")
    holder = lax.axis_index("mat")
    total[...] = jnp.zeros_like(total)

    def add(s, carry):
        total[local_row(firsts[s], holder, holders)] += arrived[s].astype(jnp.float32)
        return carry

    lax.fori_loop(0, sources, add, 0)

    def store(t, carry):
        for o in range(span):
            out[t, o] = (total[t, o] * live[o, t].astype(jnp.float32)).astype(jnp.bfloat16)
        return carry

    lax.fori_loop(0, local, store, 0)


def finish(firsts, live, arrived):
    shape = (live.shape[1],) + arrived.shape[1:]
    smem = pl.BlockSpec(memory_space=pltpu.SMEM)
    vmem = pl.BlockSpec(memory_space=pltpu.VMEM)
    return pl.pallas_call(
        finish_kernel,
        out_shape=jax.ShapeDtypeStruct(shape, jnp.bfloat16),
        in_specs=[smem, smem, vmem],
        out_specs=vmem,
        scratch_shapes=[pltpu.VMEM(shape, jnp.float32)],
        compiler_params=pltpu.CompilerParams(vmem_limit_bytes=24 * MIB),
        name="finish",
    )(firsts, live, arrived)


def far_first(count):
    return sorted(range(1, count), key=lambda s: abs(2 * s - count))


def per_device(basis_values, weights, density, block_live, batch_blocks, live_functions):
    holders = lax.axis_size("mat")
    groups = lax.axis_size("grp")
    blocks = batch_blocks.T
    live = block_live.T
    mine = jnp.arange(holders) == lax.axis_index("mat")
    largest = jnp.iinfo(jnp.int32).max
    own = jnp.min(jnp.where(mine[:, None, None], blocks[None], largest), axis=(1, 2))
    firsts = lax.pmin(own, "mat")
    rows = pick_rows(firsts, live, density)
    parts = [rows[0]] + [None] * (holders - 1)
    for s in far_first(holders):
        parts[s] = lax.ppermute(rows[s], "mat", [(h, (h + s) % holders) for h in range(holders)])
    turned = turn_values(live_functions, basis_values)
    my_group = jnp.arange(groups) == lax.axis_index("grp")
    all_firsts = lax.psum(jnp.where(my_group[:, None], firsts[None], 0).reshape(-1), "grp")
    site_density, pieces = integrate(groups, blocks, turned, weights, parts)
    arrived = lax.all_to_all(pieces, ("grp", "mat"), split_axis=0, concat_axis=0, tiled=True)
    hamiltonian = finish(all_firsts, live, arrived)
    return site_density, hamiltonian


def solution(mesh):
    in_specs = (
        P(("grp", "mat"), None, None),
        P(("grp", "mat"), None),
        P("mat", None, None, None),
        P("mat", None),
        P(("grp", "mat"), None),
        P(("grp", "mat")),
    )
    out_specs = (P(("grp", "mat"), None), P("mat", None, "grp", None))
    return jax.shard_map(
        per_device, mesh=mesh, in_specs=in_specs, out_specs=out_specs, check_vma=False
    )
```

```python
import functools

import jax
import jax.numpy as jnp
from jax import lax
from jax.experimental import pallas as pl
from jax.experimental.pallas import tpu as pltpu
from jax.sharding import PartitionSpec as P


MIB = 1 << 20
PICK_LIMIT = 62 * MIB


def far_first(count):
    return sorted(range(1, count), key=lambda s: abs(2 * s - count))


def local_row(first, holder, holders):
    return lax.div(first + lax.rem(holder - lax.rem(first, holders) + holders, holders), holders)


def pick_kernel(firsts, live, density, *refs):
    outs, held, sems = refs[:-2], refs[-2], refs[-1]
    count = len(outs)
    holder = lax.axis_index("mat")
    rows = [local_row(firsts[lax.rem(holder + s, count)], holder, count) for s in range(count)]
    order = far_first(count) + [0]
    reads = [
        pltpu.make_async_copy(density.at[rows[s]], held.at[s], sems.at[0, s]) for s in range(count)
    ]
    writes = [pltpu.make_async_copy(held.at[s], outs[s], sems.at[1, s]) for s in range(count)]
    for s in order:
        reads[s].start()
    for s in order:
        reads[s].wait()
        for o in range(density.shape[1]):
            factor = (live[o, rows[s]] * (1 if o == 0 else 2)).astype(jnp.float32)
            held[s, o] = held[s, o] * factor.astype(jnp.bfloat16)
        writes[s].start()
    for s in order:
        writes[s].wait()


def pick_rows(firsts, live, density):
    count = firsts.shape[0]
    smem = pl.BlockSpec(memory_space=pltpu.SMEM)
    hbm = pl.BlockSpec(memory_space=pltpu.HBM)
    return pl.pallas_call(
        pick_kernel,
        out_shape=(jax.ShapeDtypeStruct(density.shape[1:], jnp.bfloat16),) * count,
        in_specs=[smem, smem, hbm],
        out_specs=(hbm,) * count,
        scratch_shapes=[
            pltpu.VMEM((count,) + density.shape[1:], jnp.bfloat16),
            pltpu.SemaphoreType.DMA((2, count)),
        ],
        compiler_params=pltpu.CompilerParams(vmem_limit_bytes=PICK_LIMIT),
        name="pick",
    )(firsts, live, density)


def turn_kernel(live, values, out):
    batch = pl.program_id(0)
    turned = values[0].T
    index = lax.broadcasted_iota(jnp.int32, turned.shape, 0)
    out[0] = jnp.where(index < live[batch], turned, jnp.zeros_like(turned))


def turn_values(live, values):
    batches, points, width = values.shape
    return pl.pallas_call(
        turn_kernel,
        out_shape=jax.ShapeDtypeStruct((batches, width, points), jnp.bfloat16),
        grid_spec=pltpu.PrefetchScalarGridSpec(
            num_scalar_prefetch=1,
            grid=(batches,),
            in_specs=[pl.BlockSpec((1, points, width), lambda b, live: (b, 0, 0))],
            out_specs=pl.BlockSpec((1, width, points), lambda b, live: (b, 0, 0)),
        ),
        compiler_params=pltpu.CompilerParams(vmem_limit_bytes=16 * MIB),
        cost_estimate=pl.CostEstimate(
            flops=20_000_000_000, bytes_accessed=4 * batches * points * width, transcendentals=0
        ),
        name="turn",
    )(live, values)


def unroll_of(batches):
    return next(u for u in (8, 4, 2, 1) if batches % u == 0)


def join(rows):
    return jnp.concatenate([jnp.concatenate(row, axis=1) for row in rows], axis=0)


def integrate_kernel(groups, blocks, turned, weights, *refs):
    parts = refs[:-7]
    site_out, pieces, region, total, potential, packed, sems = refs[-7:]
    holders, span, block, _ = region.shape
    batches, width, _ = turned.shape
    slots = width // block
    half = width // 2
    pairs = [(k, l) for k in range(slots) for l in range(k, slots)]
    holder = lax.axis_index("mat")
    for s in range(holders):
        region[lax.rem(holder - s + holders, holders)] = parts[s][...]
    total[...] = jnp.zeros_like(total)
    zero = jnp.zeros((block, block), jnp.bfloat16)

    def where_is(b):
        ids = [blocks[k, b] for k in range(slots)]
        return ids, [lax.rem(i, holders) for i in ids]

    def density_of(b):
        ids, homes = where_is(b)

        def tiles(rows, columns):
            return join(
                [
                    [zero if k > l else region[homes[k], ids[l] - ids[k]] for l in columns]
                    for k in rows
                ]
            )

        values = turned[b]
        top = tiles(range(slots // 2), range(slots))
        low = tiles(range(slots // 2, slots), range(slots // 2, slots))
        product_top = jnp.dot(top, values, preferred_element_type=jnp.float32)
        product_low = jnp.dot(low, values[half:], preferred_element_type=jnp.float32)
        wide = values.astype(jnp.float32)
        site_out[pl.ds(b, 1), :] = jnp.sum(
            product_top * wide[:half] + product_low * wide[half:], axis=0, keepdims=True
        )

    unroll = unroll_of(batches)

    def densities(step, carry):
        for u in range(unroll):
            density_of(step * unroll + u)
        return carry

    lax.fori_loop(0, batches // unroll, densities, 0)
    site = site_out[...]
    potential[...] = weights[...] * site / jnp.sqrt(1.0 + site * site)

    def ham_of(b):
        ids, homes = where_is(b)
        values = turned[b]
        weighted = (potential[pl.ds(b, 1), :] * values.astype(jnp.float32)).astype(jnp.bfloat16)
        over_points = (((1,), (1,)), ((), ()))
        top = lax.dot_general(
            values[:half], weighted, over_points, preferred_element_type=jnp.float32
        )
        low = lax.dot_general(
            values[half:], weighted[half:], over_points, preferred_element_type=jnp.float32
        )
        for k, l in pairs:
            in_low = k * block >= half
            source, column = (low, l * block - half) if in_low else (top, l * block)
            row = k * block - half if in_low else k * block
            total[homes[k], ids[l] - ids[k]] += source[row : row + block, column : column + block]

    def hams(step, carry):
        for u in range(unroll):
            ham_of(step * unroll + u)
        return carry

    lax.fori_loop(0, batches // unroll, hams, 0)
    part = block // groups

    def write(h, g):
        there = g * holders + h
        return pltpu.make_async_copy(packed.at[there], pieces.at[there], sems.at[h, g])

    def store(h, carry):
        for g in range(groups):
            for o in range(span):
                packed[g * holders + h, o] = total[h, o, g * part : (g + 1) * part, :].astype(
                    jnp.bfloat16
                )
            write(h, g).start()
        return carry

    def drain(h, carry):
        for g in range(groups):
            write(h, g).wait()
        return carry

    lax.fori_loop(0, holders, store, 0)
    lax.fori_loop(0, holders, drain, 0)


def integrate(groups, blocks, turned, weights, parts):
    batches, _, points = turned.shape
    holders = len(parts)
    span, block, _ = parts[0].shape
    vmem = pl.BlockSpec(memory_space=pltpu.VMEM)
    pieces = jax.ShapeDtypeStruct((groups * holders, span, block // groups, block), jnp.bfloat16)
    return pl.pallas_call(
        functools.partial(integrate_kernel, groups),
        out_shape=(jax.ShapeDtypeStruct((batches, points), jnp.float32), pieces),
        in_specs=[pl.BlockSpec(memory_space=pltpu.SMEM)] + [vmem] * (2 + holders),
        out_specs=(vmem, pl.BlockSpec(memory_space=pltpu.HBM)),
        scratch_shapes=[
            pltpu.VMEM((holders, span, block, block), jnp.bfloat16),
            pltpu.VMEM((holders, span, block, block), jnp.float32),
            pltpu.VMEM((batches, points), jnp.float32),
            pltpu.VMEM(pieces.shape, jnp.bfloat16),
            pltpu.SemaphoreType.DMA((holders, groups)),
        ],
        compiler_params=pltpu.CompilerParams(vmem_limit_bytes=36 * MIB),
        cost_estimate=pl.CostEstimate(
            flops=5_000_000_000, bytes_accessed=8_000_000, transcendentals=0
        ),
        name="integrate",
    )(blocks, turned, weights, *parts)


def finish_kernel(firsts, live, arrived, out, total, held, sems):
    sources, span = arrived.shape[0], arrived.shape[1]
    local = out.shape[0]
    holders = lax.axis_size("mat")
    holder = lax.axis_index("mat")
    total[...] = jnp.zeros_like(total)

    def add(step, carry):
        for u in range(4):
            s = step * 4 + u
            total[local_row(firsts[s], holder, holders)] += arrived[s].astype(jnp.float32)
        return carry

    lax.fori_loop(0, sources // 4, add, 0)
    chunk = local // sems.shape[0]

    def write(c):
        rows = pl.ds(c * chunk, chunk)
        return pltpu.make_async_copy(held.at[rows], out.at[rows], sems.at[c])

    def store(c, carry):
        for u in range(chunk):
            t = c * chunk + u
            for o in range(span):
                held[t, o] = (total[t, o] * live[o, t].astype(jnp.float32)).astype(jnp.bfloat16)
        write(c).start()
        return carry

    def drain(c, carry):
        write(c).wait()
        return carry

    lax.fori_loop(0, sems.shape[0], store, 0)
    lax.fori_loop(0, sems.shape[0], drain, 0)


def finish(firsts, live, arrived):
    local = live.shape[1]
    shape = (local,) + arrived.shape[1:]
    chunk = next(c for c in (4, 3, 2, 1) if local % c == 0)
    smem = pl.BlockSpec(memory_space=pltpu.SMEM)
    return pl.pallas_call(
        finish_kernel,
        out_shape=jax.ShapeDtypeStruct(shape, jnp.bfloat16),
        in_specs=[smem, smem, pl.BlockSpec(memory_space=pltpu.VMEM)],
        out_specs=pl.BlockSpec(memory_space=pltpu.HBM),
        scratch_shapes=[
            pltpu.VMEM(shape, jnp.float32),
            pltpu.VMEM(shape, jnp.bfloat16),
            pltpu.SemaphoreType.DMA((local // chunk,)),
        ],
        compiler_params=pltpu.CompilerParams(vmem_limit_bytes=24 * MIB),
        name="finish",
    )(firsts, live, arrived)


def per_device(basis_values, weights, density, block_live, batch_blocks, live_functions):
    holders = lax.axis_size("mat")
    groups = lax.axis_size("grp")
    blocks = batch_blocks.T
    live = block_live.T
    mine = jnp.arange(holders) == lax.axis_index("mat")
    largest = jnp.iinfo(jnp.int32).max
    own = jnp.min(jnp.where(mine[:, None, None], blocks[None], largest), axis=(1, 2))
    firsts = lax.pmin(own, "mat")
    rows = pick_rows(firsts, live, density)
    parts = [rows[0]] + [None] * (holders - 1)
    for s in far_first(holders):
        parts[s] = lax.ppermute(rows[s], "mat", [(h, (h + s) % holders) for h in range(holders)])
    turned = turn_values(live_functions, basis_values)
    my_group = jnp.arange(groups) == lax.axis_index("grp")
    all_firsts = lax.psum(jnp.where(my_group[:, None], firsts[None], 0).reshape(-1), "grp")
    site_density, pieces = integrate(groups, blocks, turned, weights, parts)
    arrived = lax.all_to_all(pieces, ("grp", "mat"), split_axis=0, concat_axis=0, tiled=True)
    hamiltonian = finish(all_firsts, live, arrived)
    return site_density, hamiltonian


def solution(mesh):
    in_specs = (
        P(("grp", "mat"), None, None),
        P(("grp", "mat"), None),
        P("mat", None, None, None),
        P("mat", None),
        P(("grp", "mat"), None),
        P(("grp", "mat")),
    )
    out_specs = (P(("grp", "mat"), None), P("mat", None, "grp", None))
    return jax.shard_map(
        per_device, mesh=mesh, in_specs=in_specs, out_specs=out_specs, check_vma=False
    )
```

```python
import functools

import jax
import jax.numpy as jnp
from jax import lax
from jax.experimental import pallas as pl
from jax.experimental.pallas import tpu as pltpu
from jax.sharding import PartitionSpec as P


MIB = 1 << 20
PICK_LIMIT = 62 * MIB
DIAGONAL = 8


def far_first(count):
    return sorted(range(1, count), key=lambda s: abs(2 * s - count))


def local_row(first, holder, holders):
    return lax.div(first + lax.rem(holder - lax.rem(first, holders) + holders, holders), holders)


def packed_rows(span, block):
    return (span - 1) * block + block // 2 + DIAGONAL


def pack_diagonal(tile):
    block = tile.shape[0]
    half = block // 2
    row = lax.broadcasted_iota(jnp.int32, tile.shape, 0)
    column = lax.broadcasted_iota(jnp.int32, tile.shape, 1)
    both = jnp.where(row == column, tile, tile + tile.T)
    diagonal = jnp.sum(jnp.where(row == column, tile, 0.0), axis=0, keepdims=True)
    below = pltpu.roll(both[half:], half, axis=1)
    return jnp.where(column[:half] >= row[:half], both[:half], below), diagonal


def unpack_diagonal(packed, diagonal):
    half, _ = packed.shape
    row = lax.broadcasted_iota(jnp.int32, packed.shape, 0)
    column = lax.broadcasted_iota(jnp.int32, packed.shape, 1)
    top = jnp.where(column >= row, packed, 0.0)
    moved = pltpu.roll(packed, half, axis=1)
    inner = column - half
    low = jnp.where(inner == row, diagonal, jnp.where((inner >= 0) & (inner < row), moved, 0.0))
    return jnp.concatenate([top, low], axis=0)


def pick_kernel(firsts, live, density, *refs):
    outs, held, packed, sems = refs[:-3], refs[-3], refs[-2], refs[-1]
    count = len(outs)
    span, block = density.shape[1], density.shape[2]
    holder = lax.axis_index("mat")
    rows = [local_row(firsts[lax.rem(holder + s, count)], holder, count) for s in range(count)]
    order = far_first(count) + [0]
    reads = [
        pltpu.make_async_copy(density.at[rows[s]], held.at[s], sems.at[0, s]) for s in range(count)
    ]
    writes = [pltpu.make_async_copy(packed.at[s], outs[s], sems.at[1, s]) for s in range(count)]
    for s in order:
        reads[s].start()
    for s in order:
        reads[s].wait()
    base = (span - 1) * block
    for s in order:
        for o in range(1, span):
            factor = (2 * live[o, rows[s]]).astype(jnp.float32).astype(jnp.bfloat16)
            packed[s, (o - 1) * block : o * block] = held[s, o] * factor
        factor = live[0, rows[s]].astype(jnp.float32)
        half, diagonal = pack_diagonal(held[s, 0].astype(jnp.float32) * factor)
        packed[s, base : base + block // 2] = half.astype(jnp.bfloat16)
        packed[s, base + block // 2 :] = jnp.broadcast_to(diagonal, (DIAGONAL, block)).astype(
            jnp.bfloat16
        )
        writes[s].start()
    for s in order:
        writes[s].wait()


def pick_rows(firsts, live, density):
    count = firsts.shape[0]
    span, block = density.shape[1], density.shape[2]
    sent = (packed_rows(span, block), block)
    smem = pl.BlockSpec(memory_space=pltpu.SMEM)
    hbm = pl.BlockSpec(memory_space=pltpu.HBM)
    return pl.pallas_call(
        pick_kernel,
        out_shape=(jax.ShapeDtypeStruct(sent, jnp.bfloat16),) * count,
        in_specs=[smem, smem, hbm],
        out_specs=(hbm,) * count,
        scratch_shapes=[
            pltpu.VMEM((count,) + density.shape[1:], jnp.bfloat16),
            pltpu.VMEM((count,) + sent, jnp.bfloat16),
            pltpu.SemaphoreType.DMA((2, count)),
        ],
        compiler_params=pltpu.CompilerParams(vmem_limit_bytes=PICK_LIMIT),
        name="pick",
    )(firsts, live, density)


def turn_kernel(live, values, out):
    batch = pl.program_id(0)
    turned = values[0].T
    index = lax.broadcasted_iota(jnp.int32, turned.shape, 0)
    out[0] = jnp.where(index < live[batch], turned, jnp.zeros_like(turned))


def turn_values(live, values):
    batches, points, width = values.shape
    return pl.pallas_call(
        turn_kernel,
        out_shape=jax.ShapeDtypeStruct((batches, width, points), jnp.bfloat16),
        grid_spec=pltpu.PrefetchScalarGridSpec(
            num_scalar_prefetch=1,
            grid=(batches,),
            in_specs=[pl.BlockSpec((1, points, width), lambda b, live: (b, 0, 0))],
            out_specs=pl.BlockSpec((1, width, points), lambda b, live: (b, 0, 0)),
        ),
        compiler_params=pltpu.CompilerParams(vmem_limit_bytes=16 * MIB),
        cost_estimate=pl.CostEstimate(
            flops=20_000_000_000, bytes_accessed=4 * batches * points * width, transcendentals=0
        ),
        name="turn",
    )(live, values)


def unroll_of(batches):
    return next(u for u in (8, 4, 2, 1) if batches % u == 0)


def join(rows):
    return jnp.concatenate([jnp.concatenate(row, axis=1) for row in rows], axis=0)


def integrate_kernel(groups, blocks, turned, weights, *refs):
    parts = refs[:-5]
    site_out, pieces, region, total, potential = refs[-5:]
    holders, span, block, _ = region.shape
    batches, width, _ = turned.shape
    slots = width // block
    half = width // 2
    pairs = [(k, l) for k in range(slots) for l in range(k, slots)]
    holder = lax.axis_index("mat")
    base = (span - 1) * block
    for s in range(holders):
        home = lax.rem(holder - s + holders, holders)
        for o in range(1, span):
            region[home, o] = parts[s][(o - 1) * block : o * block]
        region[home, 0] = unpack_diagonal(
            parts[s][base : base + block // 2].astype(jnp.float32),
            parts[s][base + block // 2 :].astype(jnp.float32)[:1],
        ).astype(jnp.bfloat16)
    total[...] = jnp.zeros_like(total)
    zero = jnp.zeros((block, block), jnp.bfloat16)

    def where_is(b):
        ids = [blocks[k, b] for k in range(slots)]
        return ids, [lax.rem(i, holders) for i in ids]

    def density_of(b):
        ids, homes = where_is(b)

        def tiles(rows, columns):
            return join(
                [
                    [zero if k > l else region[homes[k], ids[l] - ids[k]] for l in columns]
                    for k in rows
                ]
            )

        values = turned[b]
        top = tiles(range(slots // 2), range(slots))
        low = tiles(range(slots // 2, slots), range(slots // 2, slots))
        product_top = jnp.dot(top, values, preferred_element_type=jnp.float32)
        product_low = jnp.dot(low, values[half:], preferred_element_type=jnp.float32)
        wide = values.astype(jnp.float32)
        site_out[pl.ds(b, 1), :] = jnp.sum(
            product_top * wide[:half] + product_low * wide[half:], axis=0, keepdims=True
        )

    unroll = unroll_of(batches)

    def densities(step, carry):
        for u in range(unroll):
            density_of(step * unroll + u)
        return carry

    lax.fori_loop(0, batches // unroll, densities, 0)
    site = site_out[...]
    potential[...] = weights[...] * site / jnp.sqrt(1.0 + site * site)

    def ham_of(b):
        ids, homes = where_is(b)
        values = turned[b]
        weighted = (potential[pl.ds(b, 1), :] * values.astype(jnp.float32)).astype(jnp.bfloat16)
        over_points = (((1,), (1,)), ((), ()))
        top = lax.dot_general(
            values[:half], weighted, over_points, preferred_element_type=jnp.float32
        )
        low = lax.dot_general(
            values[half:], weighted[half:], over_points, preferred_element_type=jnp.float32
        )
        for k, l in pairs:
            in_low = k * block >= half
            source, column = (low, l * block - half) if in_low else (top, l * block)
            row = k * block - half if in_low else k * block
            total[homes[k], ids[l] - ids[k]] += source[row : row + block, column : column + block]

    def hams(step, carry):
        for u in range(unroll):
            ham_of(step * unroll + u)
        return carry

    lax.fori_loop(0, batches // unroll, hams, 0)
    part = block // groups

    def store(h, carry):
        for g in range(groups):
            for o in range(span):
                pieces[g * holders + h, o] = total[h, o, g * part : (g + 1) * part, :].astype(
                    jnp.bfloat16
                )
        return carry

    lax.fori_loop(0, holders, store, 0)


def integrate(groups, span, blocks, turned, weights, parts):
    batches, _, points = turned.shape
    holders = len(parts)
    block = parts[0].shape[1]
    vmem = pl.BlockSpec(memory_space=pltpu.VMEM)
    pieces = jax.ShapeDtypeStruct((groups * holders, span, block // groups, block), jnp.bfloat16)
    return pl.pallas_call(
        functools.partial(integrate_kernel, groups),
        out_shape=(jax.ShapeDtypeStruct((batches, points), jnp.float32), pieces),
        in_specs=[pl.BlockSpec(memory_space=pltpu.SMEM)] + [vmem] * (2 + holders),
        out_specs=(vmem, vmem),
        scratch_shapes=[
            pltpu.VMEM((holders, span, block, block), jnp.bfloat16),
            pltpu.VMEM((holders, span, block, block), jnp.float32),
            pltpu.VMEM((batches, points), jnp.float32),
        ],
        compiler_params=pltpu.CompilerParams(vmem_limit_bytes=36 * MIB),
        cost_estimate=pl.CostEstimate(
            flops=5_000_000_000, bytes_accessed=8_000_000, transcendentals=0
        ),
        name="integrate",
    )(blocks, turned, weights, *parts)


def finish_kernel(firsts, live, arrived, out, total, held, sems):
    sources, span = arrived.shape[0], arrived.shape[1]
    local = out.shape[0]
    holders = lax.axis_size("mat")
    holder = lax.axis_index("mat")
    total[...] = jnp.zeros_like(total)

    def add(step, carry):
        for u in range(4):
            s = step * 4 + u
            total[local_row(firsts[s], holder, holders)] += arrived[s].astype(jnp.float32)
        return carry

    lax.fori_loop(0, sources // 4, add, 0)
    chunk = local // sems.shape[0]

    def write(c):
        rows = pl.ds(c * chunk, chunk)
        return pltpu.make_async_copy(held.at[rows], out.at[rows], sems.at[c])

    def store(c, carry):
        for u in range(chunk):
            t = c * chunk + u
            for o in range(span):
                held[t, o] = (total[t, o] * live[o, t].astype(jnp.float32)).astype(jnp.bfloat16)
        write(c).start()
        return carry

    def drain(c, carry):
        write(c).wait()
        return carry

    lax.fori_loop(0, sems.shape[0], store, 0)
    lax.fori_loop(0, sems.shape[0], drain, 0)


def finish(firsts, live, arrived):
    local = live.shape[1]
    shape = (local,) + arrived.shape[1:]
    chunk = next(c for c in (4, 3, 2, 1) if local % c == 0)
    smem = pl.BlockSpec(memory_space=pltpu.SMEM)
    return pl.pallas_call(
        finish_kernel,
        out_shape=jax.ShapeDtypeStruct(shape, jnp.bfloat16),
        in_specs=[smem, smem, pl.BlockSpec(memory_space=pltpu.VMEM)],
        out_specs=pl.BlockSpec(memory_space=pltpu.HBM),
        scratch_shapes=[
            pltpu.VMEM(shape, jnp.float32),
            pltpu.VMEM(shape, jnp.bfloat16),
            pltpu.SemaphoreType.DMA((local // chunk,)),
        ],
        compiler_params=pltpu.CompilerParams(vmem_limit_bytes=24 * MIB),
        name="finish",
    )(firsts, live, arrived)


def per_device(basis_values, weights, density, block_live, batch_blocks, live_functions):
    holders = lax.axis_size("mat")
    groups = lax.axis_size("grp")
    blocks = batch_blocks.T
    live = block_live.T
    mine = jnp.arange(holders) == lax.axis_index("mat")
    largest = jnp.iinfo(jnp.int32).max
    own = jnp.min(jnp.where(mine[:, None, None], blocks[None], largest), axis=(1, 2))
    firsts = lax.pmin(own, "mat")
    rows = pick_rows(firsts, live, density)
    parts = [rows[0]] + [None] * (holders - 1)
    for s in far_first(holders):
        parts[s] = lax.ppermute(rows[s], "mat", [(h, (h + s) % holders) for h in range(holders)])
    turned = turn_values(live_functions, basis_values)
    my_group = jnp.arange(groups) == lax.axis_index("grp")
    all_firsts = lax.psum(jnp.where(my_group[:, None], firsts[None], 0).reshape(-1), "grp")
    site_density, pieces = integrate(
        groups, density.shape[1], blocks, turned, weights, parts
    )
    arrived = lax.all_to_all(pieces, ("grp", "mat"), split_axis=0, concat_axis=0, tiled=True)
    hamiltonian = finish(all_firsts, live, arrived)
    return site_density, hamiltonian


def solution(mesh):
    in_specs = (
        P(("grp", "mat"), None, None),
        P(("grp", "mat"), None),
        P("mat", None, None, None),
        P("mat", None),
        P(("grp", "mat"), None),
        P(("grp", "mat")),
    )
    out_specs = (P(("grp", "mat"), None), P("mat", None, "grp", None))
    return jax.shard_map(
        per_device, mesh=mesh, in_specs=in_specs, out_specs=out_specs, check_vma=False
    )
```

```python
import functools

import jax
import jax.numpy as jnp
from jax import lax
from jax.experimental import pallas as pl
from jax.experimental.pallas import tpu as pltpu
from jax.sharding import PartitionSpec as P


MIB = 1 << 20
PICK_LIMIT = 50 * MIB
EARLY = 2
DIAGONAL = 8


def far_first(count):
    return sorted(range(1, count), key=lambda s: abs(2 * s - count))


def local_row(first, holder, holders):
    return lax.div(first + lax.rem(holder - lax.rem(first, holders) + holders, holders), holders)


def packed_rows(span, block):
    return (span - 1) * block + block // 2 + DIAGONAL


def pack_diagonal(tile):
    block = tile.shape[0]
    half = block // 2
    row = lax.broadcasted_iota(jnp.int32, tile.shape, 0)
    column = lax.broadcasted_iota(jnp.int32, tile.shape, 1)
    both = jnp.where(row == column, tile, tile + tile.T)
    diagonal = jnp.sum(jnp.where(row == column, tile, 0.0), axis=0, keepdims=True)
    below = pltpu.roll(both[half:], half, axis=1)
    return jnp.where(column[:half] >= row[:half], both[:half], below), diagonal


def unpack_diagonal(packed, diagonal):
    half, _ = packed.shape
    row = lax.broadcasted_iota(jnp.int32, packed.shape, 0)
    column = lax.broadcasted_iota(jnp.int32, packed.shape, 1)
    top = jnp.where(column >= row, packed, 0.0)
    moved = pltpu.roll(packed, half, axis=1)
    inner = column - half
    low = jnp.where(inner == row, diagonal, jnp.where((inner >= 0) & (inner < row), moved, 0.0))
    return jnp.concatenate([top, low], axis=0)


def pick_kernel(count, shifts, firsts, live, density, *refs):
    outs, held, sems = refs[:-2], refs[-2], refs[-1]
    span, block = density.shape[1], density.shape[2]
    holder = lax.axis_index("mat")
    rows = [local_row(firsts[lax.rem(holder + s, count)], holder, count) for s in shifts]
    reads = [
        pltpu.make_async_copy(density.at[row], held.at[i], sems.at[i]) for i, row in enumerate(rows)
    ]
    for read in reads:
        read.start()
    for read in reads:
        read.wait()
    base = (span - 1) * block
    for i, row in enumerate(rows):
        for o in range(1, span):
            factor = (2 * live[o, row]).astype(jnp.float32).astype(jnp.bfloat16)
            outs[i][(o - 1) * block : o * block] = held[i, o] * factor
        factor = live[0, row].astype(jnp.float32)
        half, diagonal = pack_diagonal(held[i, 0].astype(jnp.float32) * factor)
        outs[i][base : base + block // 2] = half.astype(jnp.bfloat16)
        outs[i][base + block // 2 :] = jnp.broadcast_to(diagonal, (DIAGONAL, block)).astype(
            jnp.bfloat16
        )


def pick_rows(shifts, firsts, live, density):
    span, block = density.shape[1], density.shape[2]
    smem = pl.BlockSpec(memory_space=pltpu.SMEM)
    vmem = pl.BlockSpec(memory_space=pltpu.VMEM)
    sent = jax.ShapeDtypeStruct((packed_rows(span, block), block), jnp.bfloat16)
    outs = pl.pallas_call(
        functools.partial(pick_kernel, firsts.shape[0], shifts),
        out_shape=(sent,) * len(shifts),
        in_specs=[smem, smem, pl.BlockSpec(memory_space=pltpu.HBM)],
        out_specs=(vmem,) * len(shifts),
        scratch_shapes=[
            pltpu.VMEM((len(shifts),) + density.shape[1:], jnp.bfloat16),
            pltpu.SemaphoreType.DMA((len(shifts),)),
        ],
        compiler_params=pltpu.CompilerParams(vmem_limit_bytes=PICK_LIMIT),
        name="pick",
    )(firsts, live, density)
    return dict(zip(shifts, outs))


def turn_kernel(live, values, out):
    batch = pl.program_id(0)
    turned = values[0].T
    index = lax.broadcasted_iota(jnp.int32, turned.shape, 0)
    out[0] = jnp.where(index < live[batch], turned, jnp.zeros_like(turned))


def turn_values(live, values):
    batches, points, width = values.shape
    return pl.pallas_call(
        turn_kernel,
        out_shape=jax.ShapeDtypeStruct((batches, width, points), jnp.bfloat16),
        grid_spec=pltpu.PrefetchScalarGridSpec(
            num_scalar_prefetch=1,
            grid=(batches,),
            in_specs=[pl.BlockSpec((1, points, width), lambda b, live: (b, 0, 0))],
            out_specs=pl.BlockSpec((1, width, points), lambda b, live: (b, 0, 0)),
        ),
        compiler_params=pltpu.CompilerParams(vmem_limit_bytes=16 * MIB),
        cost_estimate=pl.CostEstimate(
            flops=20_000_000_000, bytes_accessed=4 * batches * points * width, transcendentals=0
        ),
        name="turn",
    )(live, values)


def unroll_of(batches):
    return next(u for u in (8, 4, 2, 1) if batches % u == 0)


def join(rows):
    return jnp.concatenate([jnp.concatenate(row, axis=1) for row in rows], axis=0)


def integrate_kernel(groups, blocks, turned, weights, *refs):
    parts = refs[:-5]
    site_out, pieces, region, total, potential = refs[-5:]
    holders, span, block, _ = region.shape
    batches, width, _ = turned.shape
    slots = width // block
    half = width // 2
    pairs = [(k, l) for k in range(slots) for l in range(k, slots)]
    holder = lax.axis_index("mat")
    base = (span - 1) * block
    for s in range(holders):
        home = lax.rem(holder - s + holders, holders)
        for o in range(1, span):
            region[home, o] = parts[s][(o - 1) * block : o * block]
        region[home, 0] = unpack_diagonal(
            parts[s][base : base + block // 2].astype(jnp.float32),
            parts[s][base + block // 2 :].astype(jnp.float32)[:1],
        ).astype(jnp.bfloat16)
    total[...] = jnp.zeros_like(total)
    zero = jnp.zeros((block, block), jnp.bfloat16)

    def where_is(b):
        ids = [blocks[k, b] for k in range(slots)]
        return ids, [lax.rem(i, holders) for i in ids]

    def density_of(b):
        ids, homes = where_is(b)

        def tiles(rows, columns):
            return join(
                [
                    [zero if k > l else region[homes[k], ids[l] - ids[k]] for l in columns]
                    for k in rows
                ]
            )

        values = turned[b]
        top = tiles(range(slots // 2), range(slots))
        low = tiles(range(slots // 2, slots), range(slots // 2, slots))
        product_top = jnp.dot(top, values, preferred_element_type=jnp.float32)
        product_low = jnp.dot(low, values[half:], preferred_element_type=jnp.float32)
        wide = values.astype(jnp.float32)
        site_out[pl.ds(b, 1), :] = jnp.sum(
            product_top * wide[:half] + product_low * wide[half:], axis=0, keepdims=True
        )

    unroll = unroll_of(batches)

    def densities(step, carry):
        for u in range(unroll):
            density_of(step * unroll + u)
        return carry

    lax.fori_loop(0, batches // unroll, densities, 0)
    site = site_out[...]
    potential[...] = weights[...] * site / jnp.sqrt(1.0 + site * site)

    def ham_of(b):
        ids, homes = where_is(b)
        values = turned[b]
        weighted = (potential[pl.ds(b, 1), :] * values.astype(jnp.float32)).astype(jnp.bfloat16)
        over_points = (((1,), (1,)), ((), ()))
        top = lax.dot_general(
            values[:half], weighted, over_points, preferred_element_type=jnp.float32
        )
        low = lax.dot_general(
            values[half:], weighted[half:], over_points, preferred_element_type=jnp.float32
        )
        for k, l in pairs:
            in_low = k * block >= half
            source, column = (low, l * block - half) if in_low else (top, l * block)
            row = k * block - half if in_low else k * block
            total[homes[k], ids[l] - ids[k]] += source[row : row + block, column : column + block]

    def hams(step, carry):
        for u in range(unroll):
            ham_of(step * unroll + u)
        return carry

    lax.fori_loop(0, batches // unroll, hams, 0)
    part = block // groups

    def store(h, carry):
        for g in range(groups):
            for o in range(span):
                pieces[g * holders + h, o] = total[h, o, g * part : (g + 1) * part, :].astype(
                    jnp.bfloat16
                )
        return carry

    lax.fori_loop(0, holders, store, 0)


def integrate(groups, span, blocks, turned, weights, parts):
    batches, _, points = turned.shape
    holders = len(parts)
    block = parts[0].shape[1]
    vmem = pl.BlockSpec(memory_space=pltpu.VMEM)
    pieces = jax.ShapeDtypeStruct((groups * holders, span, block // groups, block), jnp.bfloat16)
    return pl.pallas_call(
        functools.partial(integrate_kernel, groups),
        out_shape=(jax.ShapeDtypeStruct((batches, points), jnp.float32), pieces),
        in_specs=[pl.BlockSpec(memory_space=pltpu.SMEM)] + [vmem] * (2 + holders),
        out_specs=(vmem, vmem),
        scratch_shapes=[
            pltpu.VMEM((holders, span, block, block), jnp.bfloat16),
            pltpu.VMEM((holders, span, block, block), jnp.float32),
            pltpu.VMEM((batches, points), jnp.float32),
        ],
        compiler_params=pltpu.CompilerParams(vmem_limit_bytes=36 * MIB),
        cost_estimate=pl.CostEstimate(
            flops=5_000_000_000, bytes_accessed=8_000_000, transcendentals=0
        ),
        name="integrate",
    )(blocks, turned, weights, *parts)


def finish_kernel(live, arrived, *refs):
    firsts, (out, total, held, sems) = refs[:-4], refs[-4:]
    span = arrived.shape[1]
    local = out.shape[0]
    holders, groups = lax.axis_size("mat"), len(firsts)
    holder, group = lax.axis_index("mat"), lax.axis_index("grp")
    total[...] = jnp.zeros_like(total)
    for s in range(groups):
        base = lax.rem(group - s + groups, groups) * holders

        def add(step, carry, s=s, base=base):
            for u in range(4):
                h = step * 4 + u
                row = local_row(firsts[s][h], holder, holders)
                total[row] += arrived[base + h].astype(jnp.float32)
            return carry

        lax.fori_loop(0, holders // 4, add, 0)
    chunk = local // sems.shape[0]

    def write(c):
        rows = pl.ds(c * chunk, chunk)
        return pltpu.make_async_copy(held.at[rows], out.at[rows], sems.at[c])

    def store(c, carry):
        for u in range(chunk):
            t = c * chunk + u
            for o in range(span):
                held[t, o] = (total[t, o] * live[o, t].astype(jnp.float32)).astype(jnp.bfloat16)
        write(c).start()
        return carry

    def drain(c, carry):
        write(c).wait()
        return carry

    lax.fori_loop(0, sems.shape[0], store, 0)
    lax.fori_loop(0, sems.shape[0], drain, 0)


def finish(firsts, live, arrived):
    local = live.shape[1]
    shape = (local,) + arrived.shape[1:]
    chunk = next(c for c in (4, 3, 2, 1) if local % c == 0)
    smem = pl.BlockSpec(memory_space=pltpu.SMEM)
    return pl.pallas_call(
        finish_kernel,
        out_shape=jax.ShapeDtypeStruct(shape, jnp.bfloat16),
        in_specs=[smem, pl.BlockSpec(memory_space=pltpu.VMEM)] + [smem] * len(firsts),
        out_specs=pl.BlockSpec(memory_space=pltpu.HBM),
        scratch_shapes=[
            pltpu.VMEM(shape, jnp.float32),
            pltpu.VMEM(shape, jnp.bfloat16),
            pltpu.SemaphoreType.DMA((local // chunk,)),
        ],
        compiler_params=pltpu.CompilerParams(vmem_limit_bytes=24 * MIB),
        name="finish",
    )(live, arrived, *firsts)


def per_device(basis_values, weights, density, block_live, batch_blocks, live_functions):
    holders = lax.axis_size("mat")
    groups = lax.axis_size("grp")
    blocks = batch_blocks.T
    live = block_live.T
    mine = jnp.arange(holders) == lax.axis_index("mat")
    largest = jnp.iinfo(jnp.int32).max
    own = jnp.min(jnp.where(mine[:, None, None], blocks[None], largest), axis=(1, 2))
    firsts = lax.pmin(own, "mat")
    shifts = far_first(holders)
    rows = pick_rows(shifts[:EARLY], firsts, live, density)
    rows |= pick_rows(shifts[EARLY:] + [0], firsts, live, density)
    parts = [rows[0]] + [None] * (holders - 1)
    for s in shifts:
        parts[s] = lax.ppermute(rows[s], "mat", [(h, (h + s) % holders) for h in range(holders)])
    turned = turn_values(live_functions, basis_values)
    all_firsts = [firsts]
    for s in range(1, groups):
        all_firsts.append(
            lax.ppermute(firsts, "grp", [(g, (g + s) % groups) for g in range(groups)])
        )
    blocks, all_firsts = lax.optimization_barrier((blocks, all_firsts))
    site_density, pieces = integrate(
        groups, density.shape[1], blocks, turned, weights, parts
    )
    arrived = lax.all_to_all(pieces, ("grp", "mat"), split_axis=0, concat_axis=0, tiled=True)
    hamiltonian = finish(all_firsts, live, arrived)
    return site_density, hamiltonian


def solution(mesh):
    in_specs = (
        P(("grp", "mat"), None, None),
        P(("grp", "mat"), None),
        P("mat", None, None, None),
        P("mat", None),
        P(("grp", "mat"), None),
        P(("grp", "mat")),
    )
    out_specs = (P(("grp", "mat"), None), P("mat", None, "grp", None))
    return jax.shard_map(
        per_device, mesh=mesh, in_specs=in_specs, out_specs=out_specs, check_vma=False
    )
```

```python
import functools

import jax
import jax.numpy as jnp
from jax import lax
from jax.experimental import pallas as pl
from jax.experimental.pallas import tpu as pltpu
from jax.sharding import PartitionSpec as P


MIB = 1 << 20
PICK_LIMIT = 50 * MIB
EARLY = 2
DIAGONAL = 8


def far_first(count):
    return sorted(range(1, count), key=lambda s: abs(2 * s - count))


def local_row(first, holder, holders):
    return lax.div(first + lax.rem(holder - lax.rem(first, holders) + holders, holders), holders)


def packed_rows(span, block):
    return (span - 1) * block + block // 2 + DIAGONAL


def pack_diagonal(tile):
    block = tile.shape[0]
    half = block // 2
    row = lax.broadcasted_iota(jnp.int32, tile.shape, 0)
    column = lax.broadcasted_iota(jnp.int32, tile.shape, 1)
    both = jnp.where(row == column, tile, tile + tile.T)
    diagonal = jnp.sum(jnp.where(row == column, tile, 0.0), axis=0, keepdims=True)
    below = pltpu.roll(both[half:], half, axis=1)
    return jnp.where(column[:half] >= row[:half], both[:half], below), diagonal


def unpack_diagonal(packed, diagonal):
    half, _ = packed.shape
    row = lax.broadcasted_iota(jnp.int32, packed.shape, 0)
    column = lax.broadcasted_iota(jnp.int32, packed.shape, 1)
    top = jnp.where(column >= row, packed, 0.0)
    moved = pltpu.roll(packed, half, axis=1)
    inner = column - half
    low = jnp.where(inner == row, diagonal, jnp.where((inner >= 0) & (inner < row), moved, 0.0))
    return jnp.concatenate([top, low], axis=0)


def pick_kernel(count, shifts, firsts, live, density, *refs):
    outs, held, masks, sems = refs[:-3], refs[-3], refs[-2], refs[-1]
    read_masks = pltpu.make_async_copy(live, masks, sems.at[len(shifts)])
    read_masks.start()
    span, block = density.shape[1], density.shape[2]
    holder = lax.axis_index("mat")
    rows = [local_row(firsts[lax.rem(holder + s, count)], holder, count) for s in shifts]
    reads = [
        pltpu.make_async_copy(density.at[row], held.at[i], sems.at[i]) for i, row in enumerate(rows)
    ]
    for read in reads:
        read.start()
    for read in reads:
        read.wait()
    read_masks.wait()
    base = (span - 1) * block
    for i, row in enumerate(rows):
        for o in range(1, span):
            factor = (2 * masks[o, row]).astype(jnp.float32).astype(jnp.bfloat16)
            outs[i][(o - 1) * block : o * block] = held[i, o] * factor
        factor = masks[0, row].astype(jnp.float32)
        half, diagonal = pack_diagonal(held[i, 0].astype(jnp.float32) * factor)
        outs[i][base : base + block // 2] = half.astype(jnp.bfloat16)
        outs[i][base + block // 2 :] = jnp.broadcast_to(diagonal, (DIAGONAL, block)).astype(
            jnp.bfloat16
        )


def pick_rows(shifts, firsts, live, density):
    span, block = density.shape[1], density.shape[2]
    smem = pl.BlockSpec(memory_space=pltpu.SMEM)
    vmem = pl.BlockSpec(memory_space=pltpu.VMEM)
    sent = jax.ShapeDtypeStruct((packed_rows(span, block), block), jnp.bfloat16)
    outs = pl.pallas_call(
        functools.partial(pick_kernel, firsts.shape[0], shifts),
        out_shape=(sent,) * len(shifts),
        in_specs=[smem] + [pl.BlockSpec(memory_space=pltpu.HBM)] * 2,
        out_specs=(vmem,) * len(shifts),
        scratch_shapes=[
            pltpu.VMEM((len(shifts),) + density.shape[1:], jnp.bfloat16),
            pltpu.SMEM(live.shape, jnp.int32),
            pltpu.SemaphoreType.DMA((len(shifts) + 1,)),
        ],
        compiler_params=pltpu.CompilerParams(vmem_limit_bytes=PICK_LIMIT),
        name="pick",
    )(firsts, live, density)
    return dict(zip(shifts, outs))


def turn_kernel(live, values, out):
    batch = pl.program_id(0)
    turned = values[0].T
    index = lax.broadcasted_iota(jnp.int32, turned.shape, 0)
    out[0] = jnp.where(index < live[batch], turned, jnp.zeros_like(turned))


def turn_values(live, values):
    batches, points, width = values.shape
    return pl.pallas_call(
        turn_kernel,
        out_shape=jax.ShapeDtypeStruct((batches, width, points), jnp.bfloat16),
        grid_spec=pltpu.PrefetchScalarGridSpec(
            num_scalar_prefetch=1,
            grid=(batches,),
            in_specs=[pl.BlockSpec((1, points, width), lambda b, live: (b, 0, 0))],
            out_specs=pl.BlockSpec((1, width, points), lambda b, live: (b, 0, 0)),
        ),
        compiler_params=pltpu.CompilerParams(vmem_limit_bytes=16 * MIB),
        cost_estimate=pl.CostEstimate(
            flops=20_000_000_000, bytes_accessed=4 * batches * points * width, transcendentals=0
        ),
        name="turn",
    )(live, values)


def unroll_of(batches):
    return next(u for u in (16, 8, 4, 2, 1) if batches % u == 0)


def join(rows):
    return jnp.concatenate([jnp.concatenate(row, axis=1) for row in rows], axis=0)


def integrate_kernel(groups, blocks, turned, weights, *refs):
    parts = refs[:-5]
    site_out, pieces, region, total, potential = refs[-5:]
    holders, span, block, _ = region.shape
    batches, width, _ = turned.shape
    slots = width // block
    half = width // 2
    pairs = [(k, l) for k in range(slots) for l in range(k, slots)]
    holder = lax.axis_index("mat")
    base = (span - 1) * block
    for s in range(holders):
        home = lax.rem(holder - s + holders, holders)
        for o in range(1, span):
            region[home, o] = parts[s][(o - 1) * block : o * block]
        region[home, 0] = unpack_diagonal(
            parts[s][base : base + block // 2].astype(jnp.float32),
            parts[s][base + block // 2 :].astype(jnp.float32)[:1],
        ).astype(jnp.bfloat16)
    total[...] = jnp.zeros_like(total)
    zero = jnp.zeros((block, block), jnp.bfloat16)

    def where_is(b):
        ids = [blocks[k, b] for k in range(slots)]
        return ids, [lax.rem(i, holders) for i in ids]

    def density_of(b):
        ids, homes = where_is(b)

        def tiles(rows, columns):
            return join(
                [
                    [zero if k > l else region[homes[k], ids[l] - ids[k]] for l in columns]
                    for k in rows
                ]
            )

        values = turned[b]
        top = tiles(range(slots // 2), range(slots))
        low = tiles(range(slots // 2, slots), range(slots // 2, slots))
        product_top = jnp.dot(top, values, preferred_element_type=jnp.float32)
        product_low = jnp.dot(low, values[half:], preferred_element_type=jnp.float32)
        wide = values.astype(jnp.float32)
        site_out[pl.ds(b, 1), :] = jnp.sum(
            product_top * wide[:half] + product_low * wide[half:], axis=0, keepdims=True
        )

    unroll = unroll_of(batches)

    def densities(step, carry):
        for u in range(unroll):
            density_of(step * unroll + u)
        return carry

    lax.fori_loop(0, batches // unroll, densities, 0)
    site = site_out[...]
    potential[...] = weights[...] * site / jnp.sqrt(1.0 + site * site)

    def ham_of(b):
        ids, homes = where_is(b)
        values = turned[b]
        weighted = (potential[pl.ds(b, 1), :] * values.astype(jnp.float32)).astype(jnp.bfloat16)
        over_points = (((1,), (1,)), ((), ()))
        top = lax.dot_general(
            values[:half], weighted, over_points, preferred_element_type=jnp.float32
        )
        low = lax.dot_general(
            values[half:], weighted[half:], over_points, preferred_element_type=jnp.float32
        )
        for k, l in pairs:
            in_low = k * block >= half
            source, column = (low, l * block - half) if in_low else (top, l * block)
            row = k * block - half if in_low else k * block
            total[homes[k], ids[l] - ids[k]] += source[row : row + block, column : column + block]

    def hams(step, carry):
        for u in range(unroll):
            ham_of(step * unroll + u)
        return carry

    lax.fori_loop(0, batches // unroll, hams, 0)
    part = block // groups

    def store(h, carry):
        for g in range(groups):
            for o in range(span):
                pieces[g * holders + h, o] = total[h, o, g * part : (g + 1) * part, :].astype(
                    jnp.bfloat16
                )
        return carry

    lax.fori_loop(0, holders, store, 0)


def integrate(groups, span, blocks, turned, weights, parts):
    batches, _, points = turned.shape
    holders = len(parts)
    block = parts[0].shape[1]
    vmem = pl.BlockSpec(memory_space=pltpu.VMEM)
    pieces = jax.ShapeDtypeStruct((groups * holders, span, block // groups, block), jnp.bfloat16)
    return pl.pallas_call(
        functools.partial(integrate_kernel, groups),
        out_shape=(jax.ShapeDtypeStruct((batches, points), jnp.float32), pieces),
        in_specs=[pl.BlockSpec(memory_space=pltpu.SMEM)] + [vmem] * (2 + holders),
        out_specs=(vmem, vmem),
        scratch_shapes=[
            pltpu.VMEM((holders, span, block, block), jnp.bfloat16),
            pltpu.VMEM((holders, span, block, block), jnp.float32),
            pltpu.VMEM((batches, points), jnp.float32),
        ],
        compiler_params=pltpu.CompilerParams(vmem_limit_bytes=36 * MIB),
        cost_estimate=pl.CostEstimate(
            flops=5_000_000_000, bytes_accessed=8_000_000, transcendentals=0
        ),
        name="integrate",
    )(blocks, turned, weights, *parts)


def finish_kernel(live, arrived, *refs):
    firsts, (out, total, held, sems) = refs[:-4], refs[-4:]
    span = arrived.shape[1]
    local = out.shape[0]
    holders, groups = lax.axis_size("mat"), len(firsts)
    holder, group = lax.axis_index("mat"), lax.axis_index("grp")
    total[...] = jnp.zeros_like(total)
    for s in range(groups):
        base = lax.rem(group - s + groups, groups) * holders

        def add(step, carry, s=s, base=base):
            for u in range(8):
                h = step * 8 + u
                row = local_row(firsts[s][h], holder, holders)
                total[row] += arrived[base + h].astype(jnp.float32)
            return carry

        lax.fori_loop(0, holders // 8, add, 0)
    chunk = local // sems.shape[0]

    def write(c):
        rows = pl.ds(c * chunk, chunk)
        return pltpu.make_async_copy(held.at[rows], out.at[rows], sems.at[c])

    def store(c, carry):
        for u in range(chunk):
            t = c * chunk + u
            for o in range(span):
                held[t, o] = (total[t, o] * live[o, t].astype(jnp.float32)).astype(jnp.bfloat16)
        write(c).start()
        return carry

    def drain(c, carry):
        write(c).wait()
        return carry

    lax.fori_loop(0, sems.shape[0], store, 0)
    lax.fori_loop(0, sems.shape[0], drain, 0)


def finish(firsts, live, arrived):
    local = live.shape[1]
    shape = (local,) + arrived.shape[1:]
    chunk = next(c for c in (6, 4, 3, 2, 1) if local % c == 0)
    smem = pl.BlockSpec(memory_space=pltpu.SMEM)
    return pl.pallas_call(
        finish_kernel,
        out_shape=jax.ShapeDtypeStruct(shape, jnp.bfloat16),
        in_specs=[smem, pl.BlockSpec(memory_space=pltpu.VMEM)] + [smem] * len(firsts),
        out_specs=pl.BlockSpec(memory_space=pltpu.HBM),
        scratch_shapes=[
            pltpu.VMEM(shape, jnp.float32),
            pltpu.VMEM(shape, jnp.bfloat16),
            pltpu.SemaphoreType.DMA((local // chunk,)),
        ],
        compiler_params=pltpu.CompilerParams(vmem_limit_bytes=24 * MIB),
        name="finish",
    )(live, arrived, *firsts)


def per_device(basis_values, weights, density, block_live, batch_blocks, live_functions):
    holders = lax.axis_size("mat")
    groups = lax.axis_size("grp")
    blocks = batch_blocks.T
    live = block_live.T
    mine = jnp.arange(holders) == lax.axis_index("mat")
    largest = jnp.iinfo(jnp.int32).max
    own = jnp.min(jnp.where(mine[:, None, None], blocks[None], largest), axis=(1, 2))
    firsts = lax.pmin(own, "mat")
    shifts = far_first(holders)
    rows = pick_rows(shifts[:EARLY], firsts, live, density)
    rows |= pick_rows(shifts[EARLY:] + [0], firsts, live, density)
    parts = [rows[0]] + [None] * (holders - 1)
    for s in shifts:
        parts[s] = lax.ppermute(rows[s], "mat", [(h, (h + s) % holders) for h in range(holders)])
    turned = turn_values(live_functions, basis_values)
    all_firsts = [firsts]
    for s in range(1, groups):
        all_firsts.append(
            lax.ppermute(firsts, "grp", [(g, (g + s) % groups) for g in range(groups)])
        )
    blocks, all_firsts = lax.optimization_barrier((blocks, all_firsts))
    site_density, pieces = integrate(
        groups, density.shape[1], blocks, turned, weights, parts
    )
    arrived = lax.all_to_all(pieces, ("grp", "mat"), split_axis=0, concat_axis=0, tiled=True)
    hamiltonian = finish(all_firsts, live, arrived)
    return site_density, hamiltonian


def solution(mesh):
    in_specs = (
        P(("grp", "mat"), None, None),
        P(("grp", "mat"), None),
        P("mat", None, None, None),
        P("mat", None),
        P(("grp", "mat"), None),
        P(("grp", "mat")),
    )
    out_specs = (P(("grp", "mat"), None), P("mat", None, "grp", None))
    return jax.shard_map(
        per_device, mesh=mesh, in_specs=in_specs, out_specs=out_specs, check_vma=False
    )
```

```python
import functools

import jax
import jax.numpy as jnp
from jax import lax
from jax.experimental import pallas as pl
from jax.experimental.pallas import tpu as pltpu
from jax.sharding import PartitionSpec as P


MIB = 1 << 20
PICK_LIMIT = 50 * MIB
EARLY = 2
DIAGONAL = 8


def far_first(count):
    return sorted(range(1, count), key=lambda s: (abs(2 * s - count), -s))


def local_row(first, holder, holders):
    return lax.div(first + lax.rem(holder - lax.rem(first, holders) + holders, holders), holders)


def packed_rows(span, block):
    return (span - 1) * block + block // 2 + DIAGONAL


def pack_diagonal(tile):
    block = tile.shape[0]
    half = block // 2
    row = lax.broadcasted_iota(jnp.int32, tile.shape, 0)
    column = lax.broadcasted_iota(jnp.int32, tile.shape, 1)
    both = jnp.where(row == column, tile, tile + tile.T)
    diagonal = jnp.sum(jnp.where(row == column, tile, 0.0), axis=0, keepdims=True)
    below = pltpu.roll(both[half:], half, axis=1)
    return jnp.where(column[:half] >= row[:half], both[:half], below), diagonal


def unpack_diagonal(packed, diagonal):
    half, _ = packed.shape
    row = lax.broadcasted_iota(jnp.int32, packed.shape, 0)
    column = lax.broadcasted_iota(jnp.int32, packed.shape, 1)
    top = jnp.where(column >= row, packed, 0.0)
    moved = pltpu.roll(packed, half, axis=1)
    inner = column - half
    low = jnp.where(inner == row, diagonal, jnp.where((inner >= 0) & (inner < row), moved, 0.0))
    return jnp.concatenate([top, low], axis=0)


def pick_kernel(count, shifts, firsts, live, density, *refs):
    outs, held, masks, sems = refs[:-3], refs[-3], refs[-2], refs[-1]
    read_masks = pltpu.make_async_copy(live, masks, sems.at[len(shifts)])
    read_masks.start()
    span, block = density.shape[1], density.shape[2]
    holder = lax.axis_index("mat")
    rows = [local_row(firsts[lax.rem(holder + s, count)], holder, count) for s in shifts]
    reads = [
        pltpu.make_async_copy(density.at[row], held.at[i], sems.at[i]) for i, row in enumerate(rows)
    ]
    for read in reads:
        read.start()
    for read in reads:
        read.wait()
    read_masks.wait()
    base = (span - 1) * block
    for i, row in enumerate(rows):
        for o in range(1, span):
            factor = (2 * masks[o, row]).astype(jnp.float32).astype(jnp.bfloat16)
            outs[i][(o - 1) * block : o * block] = held[i, o] * factor
        factor = masks[0, row].astype(jnp.float32)
        half, diagonal = pack_diagonal(held[i, 0].astype(jnp.float32) * factor)
        outs[i][base : base + block // 2] = half.astype(jnp.bfloat16)
        outs[i][base + block // 2 :] = jnp.broadcast_to(diagonal, (DIAGONAL, block)).astype(
            jnp.bfloat16
        )


def pick_rows(shifts, firsts, live, density):
    span, block = density.shape[1], density.shape[2]
    smem = pl.BlockSpec(memory_space=pltpu.SMEM)
    vmem = pl.BlockSpec(memory_space=pltpu.VMEM)
    sent = jax.ShapeDtypeStruct((packed_rows(span, block), block), jnp.bfloat16)
    outs = pl.pallas_call(
        functools.partial(pick_kernel, firsts.shape[0], shifts),
        out_shape=(sent,) * len(shifts),
        in_specs=[smem] + [pl.BlockSpec(memory_space=pltpu.HBM)] * 2,
        out_specs=(vmem,) * len(shifts),
        scratch_shapes=[
            pltpu.VMEM((len(shifts),) + density.shape[1:], jnp.bfloat16),
            pltpu.SMEM(live.shape, jnp.int32),
            pltpu.SemaphoreType.DMA((len(shifts) + 1,)),
        ],
        compiler_params=pltpu.CompilerParams(vmem_limit_bytes=PICK_LIMIT),
        name="pick",
    )(firsts, live, density)
    return dict(zip(shifts, outs))


def turn_kernel(live, values, out):
    batch = pl.program_id(0)
    turned = values[0].T
    index = lax.broadcasted_iota(jnp.int32, turned.shape, 0)
    out[0] = jnp.where(index < live[batch], turned, jnp.zeros_like(turned))


def turn_values(live, values):
    batches, points, width = values.shape
    return pl.pallas_call(
        turn_kernel,
        out_shape=jax.ShapeDtypeStruct((batches, width, points), jnp.bfloat16),
        grid_spec=pltpu.PrefetchScalarGridSpec(
            num_scalar_prefetch=1,
            grid=(batches,),
            in_specs=[pl.BlockSpec((1, points, width), lambda b, live: (b, 0, 0))],
            out_specs=pl.BlockSpec((1, width, points), lambda b, live: (b, 0, 0)),
        ),
        compiler_params=pltpu.CompilerParams(vmem_limit_bytes=16 * MIB),
        cost_estimate=pl.CostEstimate(
            flops=20_000_000_000, bytes_accessed=4 * batches * points * width, transcendentals=0
        ),
        name="turn",
    )(live, values)


def unroll_of(batches, holders):
    most = 16 if holders <= 8 else 4
    return next(u for u in (16, 8, 4, 2, 1) if u <= most and batches % u == 0)


def join(rows):
    return jnp.concatenate([jnp.concatenate(row, axis=1) for row in rows], axis=0)


def integrate_kernel(groups, blocks, turned, weights, *refs):
    parts = refs[:-5]
    site_out, pieces, region, total, potential = refs[-5:]
    holders, span, block, _ = region.shape
    batches, width, _ = turned.shape
    slots = width // block
    half = width // 2
    pairs = [(k, l) for k in range(slots) for l in range(k, slots)]
    holder = lax.axis_index("mat")
    base = (span - 1) * block
    for s in range(holders):
        home = lax.rem(holder - s + holders, holders)
        for o in range(1, span):
            region[home, o] = parts[s][(o - 1) * block : o * block]
        region[home, 0] = unpack_diagonal(
            parts[s][base : base + block // 2].astype(jnp.float32),
            parts[s][base + block // 2 :].astype(jnp.float32)[:1],
        ).astype(jnp.bfloat16)
    total[...] = jnp.zeros_like(total)
    zero = jnp.zeros((block, block), jnp.bfloat16)

    def where_is(b):
        ids = [blocks[k, b] for k in range(slots)]
        return ids, [lax.rem(i, holders) for i in ids]

    def density_of(b):
        ids, homes = where_is(b)

        def tiles(rows, columns):
            return join(
                [
                    [zero if k > l else region[homes[k], ids[l] - ids[k]] for l in columns]
                    for k in rows
                ]
            )

        values = turned[b]
        top = tiles(range(slots // 2), range(slots))
        low = tiles(range(slots // 2, slots), range(slots // 2, slots))
        product_top = jnp.dot(top, values, preferred_element_type=jnp.float32)
        product_low = jnp.dot(low, values[half:], preferred_element_type=jnp.float32)
        wide = values.astype(jnp.float32)
        site_out[pl.ds(b, 1), :] = jnp.sum(
            product_top * wide[:half] + product_low * wide[half:], axis=0, keepdims=True
        )

    unroll = unroll_of(batches, holders)

    def densities(step, carry):
        for u in range(unroll):
            density_of(step * unroll + u)
        return carry

    lax.fori_loop(0, batches // unroll, densities, 0)
    site = site_out[...]
    potential[...] = weights[...] * site / jnp.sqrt(1.0 + site * site)

    def ham_of(b):
        ids, homes = where_is(b)
        values = turned[b]
        weighted = (potential[pl.ds(b, 1), :] * values.astype(jnp.float32)).astype(jnp.bfloat16)
        over_points = (((1,), (1,)), ((), ()))
        top = lax.dot_general(
            values[:half], weighted, over_points, preferred_element_type=jnp.float32
        )
        low = lax.dot_general(
            values[half:], weighted[half:], over_points, preferred_element_type=jnp.float32
        )
        for k, l in pairs:
            in_low = k * block >= half
            source, column = (low, l * block - half) if in_low else (top, l * block)
            row = k * block - half if in_low else k * block
            total[homes[k], ids[l] - ids[k]] += source[row : row + block, column : column + block]

    def hams(step, carry):
        for u in range(unroll):
            ham_of(step * unroll + u)
        return carry

    lax.fori_loop(0, batches // unroll, hams, 0)
    part = block // groups

    def store(h, carry):
        for g in range(groups):
            for o in range(span):
                pieces[g * holders + h, o] = total[h, o, g * part : (g + 1) * part, :].astype(
                    jnp.bfloat16
                )
        return carry

    lax.fori_loop(0, holders, store, 0)


def integrate(groups, span, blocks, turned, weights, parts):
    batches, _, points = turned.shape
    holders = len(parts)
    block = parts[0].shape[1]
    vmem = pl.BlockSpec(memory_space=pltpu.VMEM)
    pieces = jax.ShapeDtypeStruct((groups * holders, span, block // groups, block), jnp.bfloat16)
    return pl.pallas_call(
        functools.partial(integrate_kernel, groups),
        out_shape=(jax.ShapeDtypeStruct((batches, points), jnp.float32), pieces),
        in_specs=[pl.BlockSpec(memory_space=pltpu.SMEM)] + [vmem] * (2 + holders),
        out_specs=(vmem, vmem),
        scratch_shapes=[
            pltpu.VMEM((holders, span, block, block), jnp.bfloat16),
            pltpu.VMEM((holders, span, block, block), jnp.float32),
            pltpu.VMEM((batches, points), jnp.float32),
        ],
        compiler_params=pltpu.CompilerParams(vmem_limit_bytes=36 * MIB),
        cost_estimate=pl.CostEstimate(
            flops=5_000_000_000, bytes_accessed=8_000_000, transcendentals=0
        ),
        name="integrate",
    )(blocks, turned, weights, *parts)


def finish_kernel(live, arrived, *refs):
    firsts, (out, total, held, sems) = refs[:-4], refs[-4:]
    span = arrived.shape[1]
    local = out.shape[0]
    holders, groups = lax.axis_size("mat"), len(firsts)
    holder, group = lax.axis_index("mat"), lax.axis_index("grp")
    total[...] = jnp.zeros_like(total)
    for s in range(groups):
        base = lax.rem(group - s + groups, groups) * holders

        def add(step, carry, s=s, base=base):
            for u in range(8):
                h = step * 8 + u
                row = local_row(firsts[s][h], holder, holders)
                total[row] += arrived[base + h].astype(jnp.float32)
            return carry

        lax.fori_loop(0, holders // 8, add, 0)
    chunk = local // sems.shape[0]

    def write(c):
        rows = pl.ds(c * chunk, chunk)
        return pltpu.make_async_copy(held.at[rows], out.at[rows], sems.at[c])

    def store(c, carry):
        for u in range(chunk):
            t = c * chunk + u
            for o in range(span):
                held[t, o] = (total[t, o] * live[o, t].astype(jnp.float32)).astype(jnp.bfloat16)
        write(c).start()
        return carry

    def drain(c, carry):
        write(c).wait()
        return carry

    lax.fori_loop(0, sems.shape[0], store, 0)
    lax.fori_loop(0, sems.shape[0], drain, 0)


def finish(firsts, live, arrived):
    local = live.shape[1]
    shape = (local,) + arrived.shape[1:]
    chunk = next(c for c in (6, 4, 3, 2, 1) if local % c == 0)
    smem = pl.BlockSpec(memory_space=pltpu.SMEM)
    return pl.pallas_call(
        finish_kernel,
        out_shape=jax.ShapeDtypeStruct(shape, jnp.bfloat16),
        in_specs=[smem, pl.BlockSpec(memory_space=pltpu.VMEM)] + [smem] * len(firsts),
        out_specs=pl.BlockSpec(memory_space=pltpu.HBM),
        scratch_shapes=[
            pltpu.VMEM(shape, jnp.float32),
            pltpu.VMEM(shape, jnp.bfloat16),
            pltpu.SemaphoreType.DMA((local // chunk,)),
        ],
        compiler_params=pltpu.CompilerParams(vmem_limit_bytes=24 * MIB),
        name="finish",
    )(live, arrived, *firsts)


def per_device(basis_values, weights, density, block_live, batch_blocks, live_functions):
    holders = lax.axis_size("mat")
    groups = lax.axis_size("grp")
    blocks = batch_blocks.T
    live = block_live.T
    mine = jnp.arange(holders) == lax.axis_index("mat")
    largest = jnp.iinfo(jnp.int32).max
    own = jnp.min(jnp.where(mine[:, None, None], blocks[None], largest), axis=(1, 2))
    firsts = lax.pmin(own, "mat")
    shifts = far_first(holders)
    rows = pick_rows(shifts[:EARLY], firsts, live, density)
    rows |= pick_rows(shifts[EARLY:] + [0], firsts, live, density)
    parts = [rows[0]] + [None] * (holders - 1)
    for s in shifts:
        parts[s] = lax.ppermute(rows[s], "mat", [(h, (h + s) % holders) for h in range(holders)])
    turned = turn_values(live_functions, basis_values)
    all_firsts = [firsts]
    for s in range(1, groups):
        all_firsts.append(
            lax.ppermute(firsts, "grp", [(g, (g + s) % groups) for g in range(groups)])
        )
    blocks, all_firsts = lax.optimization_barrier((blocks, all_firsts))
    site_density, pieces = integrate(
        groups, density.shape[1], blocks, turned, weights, parts
    )
    arrived = lax.all_to_all(pieces, ("grp", "mat"), split_axis=0, concat_axis=0, tiled=True)
    hamiltonian = finish(all_firsts, live, arrived)
    return site_density, hamiltonian


def solution(mesh):
    in_specs = (
        P(("grp", "mat"), None, None),
        P(("grp", "mat"), None),
        P("mat", None, None, None),
        P("mat", None),
        P(("grp", "mat"), None),
        P(("grp", "mat")),
    )
    out_specs = (P(("grp", "mat"), None), P("mat", None, "grp", None))
    return jax.shard_map(
        per_device, mesh=mesh, in_specs=in_specs, out_specs=out_specs, check_vma=False
    )
```
